512 devices in a mesh: slab: 128 (over z, y, core), sub: 4 (over x).
Axes of the slice: x: 4, y: 8, z: 8, core: 2. Of those that a mesh axis runs over, the one named last changes fastest.
Arguments:
- populations: float32 [19, 128, 128, 128], P(None, 'slab', 'sub'), may hold values from 0.5 to 1.5
- marker_cell: int32 [128, 4, 256, 128], P('slab', 'sub'), may hold values from 0 to 4095
- marker_count: int32 [128, 4, 256], P('slab', 'sub'), may hold values from 1 to 128
- particle_count: int32 [128, 4], P('slab', 'sub'), may hold values from 32 to 256, as said below
- particle_id: int32 [128, 4, 256], P('slab', 'sub'), may hold values from 0 to 32767, as said below
- owner_table: int32 [4, 128], P('sub'), may hold values from 0 to 127, as said below
- particle_velocity: float32 [128, 4, 3, 256], P('slab', 'sub'), may hold values from -0.3 to 0.3
- pair_list: int32 [128, 4, 256, 4], P('slab', 'sub'), may hold values from 0 to 255, as said below
- pair_gap: float32 [128, 4, 256, 4], P('slab', 'sub'), may hold values from 0.25 to 4
- self_coupling: bfloat16 [128, 128], replicated, may hold values from -2 to 16
- pair_coupling: bfloat16 [128, 128], replicated, may hold values from -1 to 6
Outputs:
- read: float32 [19, 128, 128, 128], P(None, 'slab', 'sub')
- marker_force: bfloat16 [128, 4, 256, 3, 128], P('slab', 'sub')
The draws below stay inside these ranges and needn't reach their ends.
Inputs may be any that keep to these rules, and one draw needn't show every extreme that they name: `particle_count`: A holder's live particles fill its first slots; in every sub index some holder has 256 live particles. `particle_id`: live slots of one sub index hold distinct ids; a live slot's particle is owned by slab index owner_table[j, id // 256] of the same sub index j. At most 2 live particles of one holder belong to one owner, and in every draw some holder sends exactly 2 to every owner. Dead slots hold arbitrary ids. `owner_table`: each row is a permutation of the slab indices. `pair_list`: A spot never names itself.
All inputs are finite; a program needn't handle non-finite values.
Results may differ from the reference program's by a relative error of at most 0.0053.
Values may be sent and summed in bfloat16 or wider, within the bound.
A program may use at most 64 MiB of HBM per device.

```python
import math
from functools import partial
import jax
import jax.numpy as jnp
from jax import lax

CX = 1
CY = 32
CZ = 128
PCAP = 256
MK = 128
NPAIR = 4
NX = 128
NY = 128
NZ = 128
N_SLAB = 128
N_SUB = 4


def ordering(key, array_shape):
    length = array_shape[-1]
    scores = jax.random.randint(key, array_shape, 0, 1 << 20) * length + jnp.arange(length, dtype=jnp.int32)
    return jnp.argsort(scores, axis=-1).astype(jnp.int32)


def routing(key):
    base_key = jax.random.fold_in(key, 7)
    key_list = jax.random.split(base_key, 6)
    levels = jax.random.randint(key_list[0], (N_SLAB, N_SUB), 0, 4)
    counts = PCAP // jnp.left_shift(jnp.int32(1), levels.astype(jnp.int32))
    busiest = jax.random.randint(key_list[1], (N_SUB,), 0, N_SLAB)
    counts = jnp.where(jnp.arange(N_SLAB)[:, None] == busiest[None, :], PCAP, counts).astype(jnp.int32)
    table = ordering(key_list[2], (N_SUB, N_SLAB))
    inverse = jnp.argsort(table, axis=1).astype(jnp.int32)
    destinations = ordering(key_list[3], (N_SLAB, N_SUB, N_SLAB))
    spots = ordering(key_list[4], (N_SLAB, N_SUB, PCAP))
    slot_index = jnp.arange(PCAP, dtype=jnp.int32)
    capacity = PCAP // N_SLAB
    owner_slab = destinations[:, :, slot_index % N_SLAB]
    turn_index = (slot_index // N_SLAB)[None, None, :]
    source_index = jnp.arange(N_SLAB, dtype=jnp.int32)[:, None, None]
    column_index = jnp.arange(N_SUB, dtype=jnp.int32)[None, :, None]
    owner_spot = spots[owner_slab, column_index, source_index * capacity + turn_index]
    block_index = inverse[column_index, owner_slab]
    identities = block_index * PCAP + owner_spot
    filler = jax.random.randint(key_list[5], (N_SLAB, N_SUB, PCAP), 0, N_SLAB * PCAP)
    identities = jnp.where(slot_index[None, None, :] < counts[:, :, None], identities, filler)
    return (counts, table, identities.astype(jnp.int32))


def draw_particle_count(key, part):
    return routing(key)[0]


def draw_owner_table(key, part):
    return routing(key)[1]


def draw_particle_id(key, part):
    return routing(key)[2]


def draw_pair_list(key, part):
    pair_key = jax.random.fold_in(key, 11)
    offsets = jax.random.randint(pair_key, (N_SLAB, N_SUB, PCAP, NPAIR), 0, PCAP - 1)
    spot_index = jnp.arange(PCAP, dtype=jnp.int32)[None, None, :, None]
    return ((spot_index + 1 + offsets) % PCAP).astype(jnp.int32)


def coupling_matrix(key, low_diag, high_diag, spread_scale, spread_bound):
    diag_key, spread_key = jax.random.split(key)
    diagonal = jax.random.uniform(diag_key, (MK,), jnp.float32, low_diag, high_diag)
    spread = jnp.clip(spread_scale * jax.random.normal(spread_key, (MK, MK), jnp.float32), -spread_bound, spread_bound)
    identity = jnp.eye(MK, dtype=jnp.float32)
    return (spread * (1.0 - identity) + jnp.diag(diagonal)).astype(jnp.bfloat16)


def draw_self_coupling(key, part):
    return coupling_matrix(jax.random.fold_in(key, 13), 8.0, 16.0, 0.5, 2.0)


def draw_pair_coupling(key, part):
    return coupling_matrix(jax.random.fold_in(key, 17), 2.0, 6.0, 0.25, 1.0)


def place_ends(values, key, smallest, high):
    longest = values.shape.index(max(values.shape))
    spots = []
    for shift in (0, 1):
        where = [jax.random.randint(jax.random.fold_in(key, axis), (), 0, length) for axis, length in enumerate(values.shape)]
        where[longest] = (where[longest] + shift) % values.shape[longest]
        spots.append(tuple(where))
    return values.at[spots[0]].set(smallest).at[spots[1]].set(high)


def steps_of(stream_key, extent, cuts, low, largest):
    def one(axis_at, shards_of):
        draws = jax.random.uniform(jax.random.fold_in(jax.random.fold_in(stream_key, 6), axis_at), (shards_of,), jnp.float32, low / len(cuts), largest / len(cuts))
        return jnp.repeat(jnp.exp(draws), extent[axis_at] // shards_of).reshape((-1,) + (1,) * (len(extent) - axis_at - 1))

    gain = one(*cuts[0])
    for cut in cuts[1:]:
        gain = gain * one(*cut)
    return gain


def scatter_about(own_key, extent, width, reach, pieces=(), kind=jnp.bfloat16):
    values = width * jax.random.normal(own_key, extent, jnp.float32)
    if pieces:
        values = values * steps_of(own_key, extent, pieces, -0.22, 0.18)
    return jnp.clip(values, -reach, reach).astype(kind)


def setup_inputs(seed: int = 0) -> dict:
    splits = jax.random.split(jax.random.key(seed), 12)
    return {
        "populations": jnp.clip(0.5 + 1.0 * jax.random.uniform(splits[0], (19, NX, NY, NZ), jnp.float32) ** steps_of(splits[0], (19, NX, NY, NZ), ((1, 128), (2, 4)), -0.2, 0.2), 0.5, 1.5),
        "marker_cell": place_ends(jax.random.randint(splits[1], (N_SLAB, N_SUB, PCAP, MK), 0, CX * CY * CZ), jax.random.fold_in(splits[1], 1), 0, (CX * CY * CZ) - 1).astype(jnp.int32),
        "marker_count": place_ends(jax.random.randint(splits[2], (N_SLAB, N_SUB, PCAP), 1, MK + 1), jax.random.fold_in(splits[2], 1), 1, MK).astype(jnp.int32),
        "particle_count": draw_particle_count(jax.random.fold_in(splits[11], 71), 0),
        "particle_id": draw_particle_id(jax.random.fold_in(splits[11], 71), 0),
        "owner_table": draw_owner_table(jax.random.fold_in(splits[11], 71), 0),
        "particle_velocity": scatter_about(splits[6], (N_SLAB, N_SUB, 3, PCAP), 0.05, 0.3, ((0, 128), (1, 4)), jnp.float32),
        "pair_list": draw_pair_list(jax.random.fold_in(splits[11], 71), 0),
        "pair_gap": jnp.clip(jnp.exp(math.log(4.0) - 2.7725887 * jax.random.uniform(splits[8], (N_SLAB, N_SUB, PCAP, NPAIR), jnp.float32) ** steps_of(splits[8], (N_SLAB, N_SUB, PCAP, NPAIR), ((0, 128), (1, 4)), -0.2, 0.2)), 0.25, 4.0),
        "self_coupling": draw_self_coupling(jax.random.fold_in(splits[11], 71), 0),
        "pair_coupling": draw_pair_coupling(jax.random.fold_in(splits[11], 71), 0),
    }


lattice_dirs = [(0, 0, 0), (1, 0, 0), (-1, 0, 0), (0, 1, 0), (0, -1, 0), (0, 0, 1), (0, 0, -1),
                (1, 1, 0), (-1, -1, 0), (1, -1, 0), (-1, 1, 0), (1, 0, 1), (-1, 0, -1),
                (1, 0, -1), (-1, 0, 1), (0, 1, 1), (0, -1, -1), (0, 1, -1), (0, -1, 1)]
lattice_weights = [1.0 / 3.0] + [1.0 / 18.0] * 6 + [1.0 / 36.0] * 12
opposite_of = [0, 2, 1, 4, 3, 6, 5, 8, 7, 10, 9, 12, 11, 14, 13, 16, 15, 18, 17]
relax_rate = 1.25


def moments(populations):
    dirs_table = jnp.array(lattice_dirs, jnp.float32)
    density = jnp.sum(populations, axis=0)
    moment = jnp.einsum("ic,i...->c...", dirs_table, populations, precision=lax.Precision.HIGHEST)
    return density, moment


def collide(populations, density, moment, body_force):
    dirs_table = jnp.array(lattice_dirs, jnp.float32)
    weight_col = jnp.array(lattice_weights, jnp.float32).reshape((19,) + (1,) * (populations.ndim - 1))
    velocity = (moment + 0.5 * body_force) / density
    along = jnp.einsum("ic,c...->i...", dirs_table, velocity, precision=lax.Precision.HIGHEST)
    push = jnp.einsum("ic,c...->i...", dirs_table, body_force, precision=lax.Precision.HIGHEST)
    speed_sq = jnp.sum(velocity * velocity, axis=0)
    work_rate = jnp.sum(velocity * body_force, axis=0)
    equilibrium = weight_col * density * (1.0 + 3.0 * along + 4.5 * along * along - 1.5 * speed_sq)
    source = (1.0 - 0.5 * relax_rate) * weight_col * (3.0 * (push - work_rate) + 9.0 * along * push)
    return populations - relax_rate * (populations - equilibrium) + source


def collide_plane(operands):
    plane_pops, plane_force = operands
    density, moment = moments(plane_pops)
    return collide(plane_pops, density, moment, plane_force)


def lubricate(owned, partner_index, partner_gap, self_coupling, pair_coupling):
    marker_width = owned.shape[-1]
    partners = owned[partner_index]
    weighted = jnp.sum(partners.astype(jnp.float32) / partner_gap[:, :, None, None], axis=1).astype(jnp.bfloat16)
    direct = jnp.dot(owned.reshape(-1, marker_width), self_coupling, preferred_element_type=jnp.float32)
    coupled = jnp.dot(weighted.reshape(-1, marker_width), pair_coupling, preferred_element_type=jnp.float32)
    return (direct + coupled).astype(jnp.bfloat16).reshape(owned.shape)


def lubricate_slab(operands, self_coupling, pair_coupling):
    owned, partner_index, partner_gap = operands
    column_fn = partial(lubricate, self_coupling=self_coupling, pair_coupling=pair_coupling)
    return jax.vmap(column_fn)(owned, partner_index, partner_gap)


def stream_one(collided, number, width_y):
    step_x, step_y, step_z = lattice_dirs[number]
    moved = jnp.roll(collided[number], (step_x, step_z), axis=(0, 2))
    if step_y == 0:
        return moved
    padded = jnp.pad(moved, ((0, 0), (1, 1), (0, 0)))
    moved = padded[:, 1 - step_y: 1 - step_y + width_y, :]
    edge_row = 0 if step_y == 1 else width_y - 1
    at_wall = (jnp.arange(width_y) == edge_row)[None, :, None]
    return jnp.where(at_wall, collided[opposite_of[number]], moved)


def reference(populations, marker_cell, marker_count, particle_count, particle_id, owner_table,
              particle_velocity, pair_list, pair_gap, self_coupling, pair_coupling):
    width_y = CY * N_SUB
    density, moment = moments(populations)
    fluid_flow = (moment / density).reshape(3, -1)
    slab_index = jnp.arange(N_SLAB, dtype=jnp.int32)[:, None, None, None]
    sub_index = jnp.arange(N_SUB, dtype=jnp.int32)[None, :, None, None]
    cell_x = slab_index * CX + marker_cell // (CY * CZ)
    cell_y = sub_index * CY + (marker_cell // CZ) % CY
    cell_z = marker_cell % CZ
    flat_cell = ((cell_x * width_y + cell_y) * CZ + cell_z).reshape(-1).astype(jnp.int32)
    sampled = jnp.take(fluid_flow, flat_cell, axis=1).reshape(3, N_SLAB, N_SUB, PCAP, MK)
    sampled = jnp.transpose(sampled, (1, 2, 3, 0, 4))
    slot_index = jnp.arange(PCAP, dtype=jnp.int32)
    alive_slot = slot_index[None, None, :] < particle_count[:, :, None]
    marker_index = jnp.arange(MK, dtype=jnp.int32)[None, None, None, :]
    live_marker = alive_slot[..., None] & (marker_index < marker_count[..., None])
    target_speed = jnp.transpose(particle_velocity, (0, 1, 3, 2))[..., None]
    slip_value = jnp.where(live_marker[:, :, :, None, :], target_speed - sampled, 0.0).astype(jnp.bfloat16)
    column_index = sub_index[..., 0]
    owner_slab = owner_table[column_index, particle_id // PCAP]
    owner_spot = particle_id % PCAP
    total_slots = N_SLAB * N_SUB * PCAP
    target_row = jnp.where(alive_slot, (owner_slab * N_SUB + column_index) * PCAP + owner_spot, total_slots)
    target_row = target_row.reshape(-1).astype(jnp.int32)
    gathered = jnp.zeros((total_slots, 3, MK), jnp.bfloat16).at[target_row].set(
        slip_value.reshape(total_slots, 3, MK), mode="drop")
    gathered = gathered.reshape(N_SLAB, N_SUB, PCAP, 3, MK)
    slab_fn = partial(lubricate_slab, self_coupling=self_coupling, pair_coupling=pair_coupling)
    correction = lax.map(slab_fn, (gathered, pair_list, pair_gap)).reshape(total_slots, 3, MK)
    returned = correction[jnp.minimum(target_row, total_slots - 1)].reshape(N_SLAB, N_SUB, PCAP, 3, MK)
    marker_force = jnp.where(live_marker[:, :, :, None, :], returned, 0.0).astype(jnp.bfloat16)
    spread_terms = jnp.transpose(marker_force.astype(jnp.float32), (3, 0, 1, 2, 4)).reshape(3, -1)
    body_force = jnp.zeros((3, N_SLAB * CX * width_y * CZ), jnp.float32).at[:, flat_cell].add(spread_terms)
    body_force = body_force.reshape(3, N_SLAB * CX, width_y, CZ)
    collided = lax.map(collide_plane, (jnp.moveaxis(populations, 1, 0), jnp.moveaxis(body_force, 1, 0)))
    collided = jnp.moveaxis(collided, 0, 1)
    read = jnp.stack([stream_one(collided, number, width_y) for number in range(19)])
    return read, marker_force
```

```python
import functools

import jax
import jax.numpy as jnp
from jax import lax
from jax.experimental import pallas as pl
from jax.experimental.pallas import tpu as pltpu
from jax.sharding import PartitionSpec as P

DIRS = [
    (0, 0, 0),
    (1, 0, 0),
    (-1, 0, 0),
    (0, 1, 0),
    (0, -1, 0),
    (0, 0, 1),
    (0, 0, -1),
    (1, 1, 0),
    (-1, -1, 0),
    (1, -1, 0),
    (-1, 1, 0),
    (1, 0, 1),
    (-1, 0, -1),
    (1, 0, -1),
    (-1, 0, 1),
    (0, 1, 1),
    (0, -1, -1),
    (0, 1, -1),
    (0, -1, 1),
]
WEIGHTS = [1.0 / 3.0] + [1.0 / 18.0] * 6 + [1.0 / 36.0] * 12
OPPOSITE = [0, 2, 1, 4, 3, 6, 5, 8, 7, 10, 9, 12, 11, 14, 13, 16, 15, 18, 17]
OMEGA = 1.25
X_UP = [i for i in range(19) if DIRS[i][0] == 1]
X_DOWN = [i for i in range(19) if DIRS[i][0] == -1]
Y_UP = [i for i in range(19) if DIRS[i][1] == 1]
Y_DOWN = [i for i in range(19) if DIRS[i][1] == -1]

F32 = jnp.float32
BF16 = jnp.bfloat16
NN = (((1,), (0,)), ((), ()))
NT = (((1,), (1,)), ((), ()))
TN = (((0,), (0,)), ((), ()))


def dot(a, b, dims=NN):
    return lax.dot_general(a, b, dims, preferred_element_type=F32)


def iota(shape, axis):
    return lax.broadcasted_iota(jnp.int32, shape, axis)


def ones_at(mask):
    return jnp.where(mask, 1.0, 0.0).astype(BF16)


def split_two(value):
    high = value.astype(BF16)
    return high, (value - high.astype(F32)).astype(BF16)


def moments(pops_ref):
    pops = [pops_ref[i] for i in range(19)]
    density = functools.reduce(lambda a, b: a + b, pops)
    moment = []
    for c in range(3):
        up = functools.reduce(lambda a, b: a + b, [pops[i] for i in range(19) if DIRS[i][c] == 1])
        down = functools.reduce(lambda a, b: a + b, [pops[i] for i in range(19) if DIRS[i][c] == -1])
        moment.append(up - down)
    return density, moment


def flow_table(pops_ref, flow_ref):
    rows = pops_ref.shape[1]
    density, moment = moments(pops_ref)
    for c in range(3):
        flow_ref[pl.ds(c * rows, rows), :] = moment[c] / density


def slot_columns(velocity_ref, mcount_ref, pcount_ref, cols_ref):
    slots = mcount_ref.shape[1]
    lim = jnp.where(iota((1, slots), 1) < pcount_ref[...], mcount_ref[...], 0).astype(F32)
    stack = [velocity_ref[...].reshape(3, slots)] if velocity_ref is not None else [jnp.zeros((3, slots), F32)]
    stack = jnp.concatenate(stack + [lim, jnp.zeros((4, slots), F32)], axis=0)
    cols_ref[...] = stack.T


def routes(pid_ref, table_ref, pcount_ref, width):
    slots, slabs = pid_ref.shape[1], table_ref.shape[1]
    ids = pid_ref[...]
    alive = iota((1, slots), 1) < pcount_ref[...]
    in_range = ones_at(iota((slabs, slots), 0) == ids // slots)
    owner_of = ones_at(iota((slabs, slabs), 0) == table_ref[...])
    owner = jnp.where(alive, dot(owner_of, in_range), 0.0)
    before = ones_at(iota((slots, slots), 0) < iota((slots, slots), 1))
    earlier = dot(owner.astype(BF16), before)
    first = jnp.where(earlier < 0.5, owner, 0.0)
    pick = jnp.concatenate([first, owner - first], axis=0).astype(BF16)
    spot = (ids % slots + 1).astype(F32)
    spots = dot(pick, jnp.broadcast_to(spot, (width, slots)).astype(BF16), NT)
    return pick, spots


def sample(cell_ref, flow_ref, cols_ref, slip_ref):
    slots, width = cell_ref.shape
    rows = flow_ref.shape[0] // 3
    depth = flow_ref.shape[1]

    def block(g, carry):
        at = pl.multiple_of(g * 8, 8)
        cell = cell_ref[pl.ds(at, 8), :]
        z = cell % depth
        y = cell // depth
        picked = [jnp.zeros((8, width), F32) for _ in range(3)]
        for row in range(rows):
            here = y == row
            for c in range(3):
                line = jnp.broadcast_to(flow_ref[c * rows + row : c * rows + row + 1, :], (8, depth))
                got = jnp.take_along_axis(line, z, axis=1, mode="promise_in_bounds")
                picked[c] = jnp.where(here, got, picked[c])
        cols = cols_ref[pl.ds(at, 8), :]
        live = iota((8, width), 1).astype(F32) < cols[:, 3:4]
        for c in range(3):
            slip_ref[c, pl.ds(at, 8), :] = jnp.where(live, cols[:, c : c + 1] - picked[c], 0.0)
        return carry

    lax.fori_loop(0, slots // 8, block, 0)


def put_rows(wide_ref, rows, width):
    slabs = wide_ref.shape[0] // 8
    for p in range(2):
        for c in range(3):
            wide_ref[pl.ds(p * 3 + c, slabs, stride=8), :] = rows[
                p * slabs : (p + 1) * slabs, c * width : (c + 1) * width
            ]


def take_rows(wide_ref):
    slabs = wide_ref.shape[0] // 8
    sides = []
    for p in range(2):
        sides.append(
            jnp.concatenate(
                [wide_ref[pl.ds(p * 3 + c, slabs, stride=8), :] for c in range(3)], axis=1
            )
        )
    return jnp.concatenate(sides, axis=0).astype(BF16)


def front_kernel(
    pops_ref, cell_ref, mcount_ref, pcount_ref, pid_ref, table_ref, velocity_ref,
    message_ref, pick_ref, flow_ref, cols_ref, slip_ref, wide_ref,
):
    slots, width = cell_ref.shape
    slabs = slots // 2
    pick, spots = routes(pid_ref, table_ref, pcount_ref, width)
    pick_ref[...] = pick
    flow_table(pops_ref, flow_ref)
    slot_columns(velocity_ref, mcount_ref, pcount_ref, cols_ref)
    sample(cell_ref, flow_ref, cols_ref, slip_ref)
    slip = jnp.concatenate([slip_ref[c].astype(BF16) for c in range(3)], axis=1)
    put_rows(wide_ref, dot(pick_ref[...], slip), width)
    for p in range(2):
        wide_ref[pl.ds(6 + p, slabs, stride=8), :] = spots[p * slabs : (p + 1) * slabs]
    message_ref[...] = wide_ref[...].reshape(slabs, 8, width).astype(BF16)


def owner_kernel(
    got_ref, partner_ref, gap_ref, self_ref, pair_ref, reply_ref, wide_ref,
):
    slabs, _, width = got_ref.shape
    slots = 2 * slabs
    wide_ref[...] = got_ref[...].astype(F32).reshape(8 * slabs, width)
    owned = take_rows(wide_ref)
    spot_col = jnp.concatenate(
        [wide_ref[pl.ds(6 + p, slabs, stride=8), :] for p in range(2)], axis=0
    )
    head = ones_at(iota((slots, width), 1) == 0)
    spot_row = dot(head, spot_col.astype(BF16), NT)
    pairs = jnp.concatenate([partner_ref[...].astype(F32), gap_ref[...]], axis=0).T
    weight = jnp.zeros((slots, slots), F32)
    for k in range(4):
        weight += jnp.where(pairs[:, k : k + 1] + 1.0 == spot_row, 1.0 / pairs[:, 4 + k : 5 + k], 0.0)
    high, low = split_two(weight)
    near = (dot(high, owned) + dot(low, owned)).astype(BF16)
    place = jnp.where(spot_col[:, :1] - 1.0 == iota((slots, slots), 1).astype(F32), 1.0, 0.0).astype(BF16)
    near = dot(place, near).astype(BF16)
    parts = []
    for c in range(3):
        side = slice(c * width, (c + 1) * width)
        parts.append(dot(owned[:, side], self_ref[...]) + dot(near[:, side], pair_ref[...]))
    put_rows(wide_ref, jnp.concatenate(parts, axis=1), width)
    reply_ref[...] = wide_ref[...].reshape(slabs, 8, width).astype(BF16)


def spread(cell_ref, force_ref, rows, depth):
    slots, width = cell_ref.shape
    high_iota = iota((16, width), 0).astype(F32).astype(BF16)

    def block(g, total):
        at = pl.multiple_of(g * 8, 8)
        cell = cell_ref[pl.ds(at, 8), :]
        zf = (cell % depth).astype(F32)
        yf = (cell // depth).astype(F32)
        vals = [force_ref[c, pl.ds(at, 8), :] for c in range(3)]

        def packed(value, j):
            return jnp.broadcast_to(value[j : j + 1, :], (16, width)).astype(BF16)

        for pair in range(4):
            a_side, b_side = [], []
            for j in (2 * pair, 2 * pair + 1):
                zb, yb = packed(zf, j), packed(yf, j)
                one, zero = jnp.ones((16, width), BF16), jnp.zeros((16, width), BF16)
                b_side.append(
                    jnp.concatenate(
                        [jnp.where(zb == high_iota + 16 * i, one, zero) for i in range(depth // 16)], axis=0
                    )
                )
                marks = [yb == high_iota + 16 * i for i in range(rows // 16)]
                lines = []
                for c in range(3):
                    vb = packed(vals[c], j)
                    lines += [jnp.where(mark, vb, zero) for mark in marks]
                a_side.append(jnp.concatenate(lines, axis=0))
            total = total + dot(jnp.concatenate(a_side, axis=1), jnp.concatenate(b_side, axis=1), NT)
        return total

    return lax.fori_loop(0, slots // 8, block, jnp.zeros((3 * rows, depth), F32))


def collide(pops_ref, force, out_ref):
    density, moment = moments(pops_ref)
    inverse = 1.0 / density
    velocity = [(moment[c] + 0.5 * force[c]) * inverse for c in range(3)]
    speed_sq = velocity[0] * velocity[0] + velocity[1] * velocity[1] + velocity[2] * velocity[2]
    work = velocity[0] * force[0] + velocity[1] * force[1] + velocity[2] * force[2]

    def along(i, parts):
        terms = [parts[c] if DIRS[i][c] == 1 else -parts[c] for c in range(3) if DIRS[i][c] != 0]
        return functools.reduce(lambda a, b: a + b, terms) if terms else None

    for i in range(19):
        w = WEIGHTS[i]
        cu, cf = along(i, velocity), along(i, force)
        base = 1.0 - 1.5 * speed_sq
        if cu is None:
            equilibrium = w * density * base
            source = (1.0 - 0.5 * OMEGA) * w * (-3.0 * work)
        else:
            equilibrium = w * density * (base + 3.0 * cu + 4.5 * cu * cu)
            source = (1.0 - 0.5 * OMEGA) * w * (3.0 * (cf - work) + 9.0 * cu * cf)
        pops = pops_ref[i]
        out_ref[i] = pops - OMEGA * (pops - equilibrium) + source


def back_kernel(
    returned_ref, pick_ref, pops_ref, cell_ref, mcount_ref, pcount_ref,
    marker_ref, collided_ref, cols_ref, force_ref, wide_ref,
):
    slots, width = cell_ref.shape
    slabs = slots // 2
    rows, depth = pops_ref.shape[1:]
    wide_ref[...] = returned_ref[...].astype(F32).reshape(8 * slabs, width)
    own = dot(pick_ref[...], take_rows(wide_ref), TN)
    slot_columns(None, mcount_ref, pcount_ref, cols_ref)
    live = iota((slots, width), 1).astype(F32) < cols_ref[:, 3:4]
    for c in range(3):
        value = jnp.where(live, own[:, c * width : (c + 1) * width], 0.0)
        force_ref[c] = value
        marker_ref[c] = value.astype(BF16)
    total = spread(cell_ref, force_ref, rows, depth)
    collide(pops_ref, [total[c * rows : (c + 1) * rows] for c in range(3)], collided_ref)


def stream(collided_ref, x_low_ref, x_high_ref, y_low_ref, y_high_ref, read_ref, sub_total):
    rows, depth = collided_ref.shape[1:]
    me = lax.axis_index("sub")
    row = iota((rows, depth), 0)
    for i in range(19):
        sx, sy, sz = DIRS[i]
        if sx == 0:
            value = collided_ref[i]
        elif sx == 1:
            value = x_low_ref[X_UP.index(i)]
        else:
            value = x_high_ref[X_DOWN.index(i)]
        if sy == 1:
            edge = y_low_ref[Y_UP.index(i)]
            value = jnp.where(row == 0, edge[0:1, :], pltpu.roll(value, 1, 0))
        elif sy == -1:
            edge = y_high_ref[Y_DOWN.index(i)]
            value = jnp.where(row == rows - 1, edge[0:1, :], pltpu.roll(value, rows - 1, 0))
        if sz != 0:
            value = pltpu.roll(value, sz % depth, 1)
        if sy != 0:
            wall_row, wall_device = (0, 0) if sy == 1 else (rows - 1, sub_total - 1)
            at_wall = (row == wall_row) & (me == wall_device)
            value = jnp.where(at_wall, collided_ref[OPPOSITE[i]], value)
        read_ref[i] = value


def vmem(n):
    return [pl.BlockSpec(memory_space=pltpu.VMEM)] * n


def call(body, outs, scratch, args, name):
    return pl.pallas_call(
        body,
        out_shape=[jax.ShapeDtypeStruct(shape, kind) for shape, kind in outs],
        in_specs=vmem(len(args)),
        out_specs=vmem(len(outs)),
        scratch_shapes=[pltpu.VMEM(shape, kind) for shape, kind in scratch],
        name=name,
    )(*args)


def per_device(
    populations, marker_cell, marker_count, particle_count, particle_id, owner_table,
    particle_velocity, pair_list, pair_gap, self_coupling, pair_coupling,
):
    rows, depth = populations.shape[2:]
    slots, width = marker_cell.shape[2:]
    slabs = lax.axis_size("slab")
    pops = populations[:, 0]
    cell = marker_cell[0, 0]
    mcount = marker_count[0]
    pid = particle_id[0]
    velocity = jnp.transpose(particle_velocity[0], (1, 0, 2))
    partners = jnp.transpose(pair_list[0, 0])
    gaps = jnp.transpose(pair_gap[0, 0])
    message, pick = call(
        front_kernel,
        [((slabs, 8, width), BF16), ((slots, slots), BF16)],
        [((3 * rows, depth), F32), ((slots, 8), F32), ((3, slots, width), F32), ((8 * slabs, width), F32)],
        (pops, cell, mcount, particle_count, pid, owner_table, velocity),
        "front",
    )
    got = lax.all_to_all(message, "slab", split_axis=0, concat_axis=0, tiled=True)
    (reply,) = call(
        owner_kernel,
        [((slabs, 8, width), BF16)],
        [((8 * slabs, width), F32)],
        (got, partners, gaps, self_coupling, pair_coupling),
        "owner",
    )
    returned = lax.all_to_all(reply, "slab", split_axis=0, concat_axis=0, tiled=True)
    marker, collided = call(
        back_kernel,
        [((3, slots, width), BF16), ((19, rows, depth), F32)],
        [((slots, 8), F32), ((3, slots, width), F32), ((8 * slabs, width), F32)],
        (returned, pick, pops, cell, mcount, particle_count),
        "back",
    )
    up = [(i, (i + 1) % slabs) for i in range(slabs)]
    down = [(b, a) for a, b in up]
    x_low = lax.ppermute(jnp.stack([collided[i] for i in X_UP]), "slab", up)
    x_high = lax.ppermute(jnp.stack([collided[i] for i in X_DOWN]), "slab", down)

    def plane(i):
        return {0: collided, 1: x_low, -1: x_high}[DIRS[i][0]][
            {0: i, 1: X_UP.index(i) if i in X_UP else 0, -1: X_DOWN.index(i) if i in X_DOWN else 0}[DIRS[i][0]]
        ]

    subs = lax.axis_size("sub")
    forward = [(i, i + 1) for i in range(subs - 1)]
    y_low = lax.ppermute(jnp.stack([plane(i)[rows - 1 :] for i in Y_UP]), "sub", forward)
    y_high = lax.ppermute(jnp.stack([plane(i)[:1] for i in Y_DOWN]), "sub", [(b, a) for a, b in forward])
    (read,) = call(
        functools.partial(stream, sub_total=subs),
        [((19, rows, depth), F32)],
        [],
        (collided, x_low, x_high, y_low, y_high),
        "stream",
    )
    return read[:, None], jnp.transpose(marker, (1, 0, 2))[None, None]


def solution(mesh):
    placed = (
        P(None, "slab", "sub", None),
        P("slab", "sub", None, None),
        P("slab", "sub", None),
        P("slab", "sub"),
        P("slab", "sub", None),
        P("sub", None),
        P("slab", "sub", None, None),
        P("slab", "sub", None, None),
        P("slab", "sub", None, None),
        P(),
        P(),
    )
    return jax.shard_map(
        per_device,
        mesh=mesh,
        in_specs=placed,
        out_specs=(P(None, "slab", "sub", None), P("slab", "sub", None, None, None)),
        check_vma=False,
    )
```

```python
import functools

import jax
import jax.numpy as jnp
from jax import lax
from jax.experimental import pallas as pl
from jax.experimental.pallas import tpu as pltpu
from jax.sharding import PartitionSpec as P

DIRS = [
    (0, 0, 0),
    (1, 0, 0),
    (-1, 0, 0),
    (0, 1, 0),
    (0, -1, 0),
    (0, 0, 1),
    (0, 0, -1),
    (1, 1, 0),
    (-1, -1, 0),
    (1, -1, 0),
    (-1, 1, 0),
    (1, 0, 1),
    (-1, 0, -1),
    (1, 0, -1),
    (-1, 0, 1),
    (0, 1, 1),
    (0, -1, -1),
    (0, 1, -1),
    (0, -1, 1),
]
WEIGHTS = [1.0 / 3.0] + [1.0 / 18.0] * 6 + [1.0 / 36.0] * 12
OPPOSITE = [0, 2, 1, 4, 3, 6, 5, 8, 7, 10, 9, 12, 11, 14, 13, 16, 15, 18, 17]
OMEGA = 1.25
X_UP = [i for i in range(19) if DIRS[i][0] == 1]
X_DOWN = [i for i in range(19) if DIRS[i][0] == -1]
Y_UP = [i for i in range(19) if DIRS[i][1] == 1]
Y_DOWN = [i for i in range(19) if DIRS[i][1] == -1]

F32 = jnp.float32
BF16 = jnp.bfloat16
NN = (((1,), (0,)), ((), ()))
NT = (((1,), (1,)), ((), ()))
TN = (((0,), (0,)), ((), ()))


def dot(a, b, dims=NN):
    return lax.dot_general(a, b, dims, preferred_element_type=F32)


def iota(shape, axis):
    return lax.broadcasted_iota(jnp.int32, shape, axis)


def ones_at(mask):
    return jnp.where(mask, 1.0, 0.0).astype(BF16)


def split_cell(cell, depth):
    return cell & (depth - 1), lax.shift_right_logical(cell, depth.bit_length() - 1)


def split_two(value):
    high = value.astype(BF16)
    return high, (value - high.astype(F32)).astype(BF16)


def moments(pops_ref):
    pops = [pops_ref[i] for i in range(19)]
    density = functools.reduce(lambda a, b: a + b, pops)
    moment = []
    for c in range(3):
        up = functools.reduce(lambda a, b: a + b, [pops[i] for i in range(19) if DIRS[i][c] == 1])
        down = functools.reduce(lambda a, b: a + b, [pops[i] for i in range(19) if DIRS[i][c] == -1])
        moment.append(up - down)
    return density, moment


def flow_table(pops_ref, flow_ref):
    rows = pops_ref.shape[1]
    density, moment = moments(pops_ref)
    for c in range(3):
        flow_ref[pl.ds(c * rows, rows), :] = moment[c] / density


def slot_columns(velocity_ref, mcount_ref, pcount_ref, cols_ref):
    slots = mcount_ref.shape[1]
    lim = jnp.where(iota((1, slots), 1) < pcount_ref[...], mcount_ref[...], 0).astype(F32)
    stack = [velocity_ref[...].reshape(3, slots)] if velocity_ref is not None else [jnp.zeros((3, slots), F32)]
    stack = jnp.concatenate(stack + [lim, jnp.zeros((4, slots), F32)], axis=0)
    cols_ref[...] = stack.T


def routes(pid_ref, table_ref, pcount_ref, width):
    slots, slabs = pid_ref.shape[1], table_ref.shape[1]
    ids = pid_ref[...]
    alive = iota((1, slots), 1) < pcount_ref[...]
    in_range = ones_at(iota((slabs, slots), 0) == ids // slots)
    owner_of = ones_at(iota((slabs, slabs), 0) == table_ref[...])
    owner = jnp.where(alive, dot(owner_of, in_range), 0.0)
    before = ones_at(iota((slots, slots), 0) < iota((slots, slots), 1))
    earlier = dot(owner.astype(BF16), before)
    first = jnp.where(earlier < 0.5, owner, 0.0)
    pick = jnp.concatenate([first, owner - first], axis=0).astype(BF16)
    spot = (ids % slots + 1).astype(F32)
    spots = dot(pick, jnp.broadcast_to(spot, (width, slots)).astype(BF16), NT)
    return pick, spots


def sample(cell_ref, flow_ref, cols_ref, slip_ref):
    slots, width = cell_ref.shape
    rows = flow_ref.shape[0] // 3
    depth = flow_ref.shape[1]

    def block(g, carry):
        at = pl.multiple_of(g * 8, 8)
        cell = cell_ref[pl.ds(at, 8), :]
        z, y = split_cell(cell, depth)
        picked = [jnp.zeros((8, width), F32) for _ in range(3)]
        for row in range(rows):
            here = y == row
            for c in range(3):
                line = jnp.broadcast_to(flow_ref[c * rows + row : c * rows + row + 1, :], (8, depth))
                got = jnp.take_along_axis(line, z, axis=1, mode="promise_in_bounds")
                picked[c] = jnp.where(here, got, picked[c])
        cols = cols_ref[pl.ds(at, 8), :]
        live = iota((8, width), 1).astype(F32) < cols[:, 3:4]
        for c in range(3):
            slip_ref[c, pl.ds(at, 8), :] = jnp.where(live, cols[:, c : c + 1] - picked[c], 0.0)
        return carry

    lax.fori_loop(0, slots // 8, block, 0)


def put_rows(wide_ref, rows, width):
    slabs = wide_ref.shape[0] // 8
    for p in range(2):
        for c in range(3):
            wide_ref[pl.ds(p * 3 + c, slabs, stride=8), :] = rows[
                p * slabs : (p + 1) * slabs, c * width : (c + 1) * width
            ]


def take_rows(wide_ref):
    slabs = wide_ref.shape[0] // 8
    sides = []
    for p in range(2):
        sides.append(
            jnp.concatenate(
                [wide_ref[pl.ds(p * 3 + c, slabs, stride=8), :] for c in range(3)], axis=1
            )
        )
    return jnp.concatenate(sides, axis=0).astype(BF16)


ORDER = X_UP + X_DOWN + [3, 4, 15, 16, 17, 18, 0, 5, 6]
PLACE = [ORDER.index(i) for i in range(19)]
EDGES = [3, 15, 17, 7, 10, 4, 16, 18, 9, 8]


def routed(mesh_ids):
    return dict(device_id=mesh_ids, device_id_type=pl.DeviceIdType.MESH)


def near_ids():
    slabs, subs = lax.axis_size("slab"), lax.axis_size("sub")
    me, side = lax.axis_index("slab"), lax.axis_index("sub")
    next_slab, last_slab = lax.rem(me + 1, slabs), lax.rem(me + slabs - 1, slabs)
    next_sub, last_sub = lax.rem(side + 1, subs), lax.rem(side + subs - 1, subs)
    return [
        {"slab": me, "sub": next_sub},
        {"slab": next_slab, "sub": next_sub},
        {"slab": last_slab, "sub": next_sub},
        {"slab": me, "sub": last_sub},
        {"slab": next_slab, "sub": last_sub},
        {"slab": last_slab, "sub": last_sub},
        {"slab": next_slab, "sub": side},
        {"slab": last_slab, "sub": side},
    ]


def greet():
    slabs = lax.axis_size("slab")
    me, side = lax.axis_index("slab"), lax.axis_index("sub")
    barrier = pltpu.get_barrier_semaphore()

    def one(k, carry):
        pl.semaphore_signal(barrier, inc=1, **routed({"slab": lax.rem(me + k, slabs), "sub": side}))
        return carry

    lax.fori_loop(1, slabs, one, 0)
    for ids in near_ids()[:6]:
        pl.semaphore_signal(barrier, inc=1, **routed(ids))


def met():
    pl.semaphore_wait(pltpu.get_barrier_semaphore(), lax.axis_size("slab") + 5)


def exchange_start(out_ref, in_ref, send_sem, recv_sem, own_sem):
    slabs = lax.axis_size("slab")
    me, side = lax.axis_index("slab"), lax.axis_index("sub")

    def one(k, carry):
        to = lax.rem(me + k, slabs)
        pltpu.make_async_remote_copy(
            src_ref=out_ref.at[to],
            dst_ref=in_ref.at[me],
            send_sem=send_sem,
            recv_sem=recv_sem,
            **routed({"slab": to, "sub": side}),
        ).start()
        return carry

    lax.fori_loop(1, slabs, one, 0)
    pltpu.make_async_copy(out_ref.at[me], in_ref.at[me], own_sem).start()


def exchange_wait(out_ref, in_ref, send_sem, recv_sem, own_sem):
    slabs = lax.axis_size("slab")
    me = lax.axis_index("slab")
    others = pl.ds(0, slabs - 1)
    pltpu.make_async_copy(out_ref.at[me], in_ref.at[me], own_sem).wait()
    pltpu.make_async_copy(in_ref.at[others], in_ref.at[others], recv_sem).wait()
    pltpu.make_async_copy(out_ref.at[others], out_ref.at[others], send_sem).wait()


def halo_copies(collided_ref, x_low_ref, x_high_ref, edge_out_ref, edge_in_ref, send_sem, recv_sem):
    ids = near_ids()
    views = [(edge_out_ref.at[pl.ds(a, n)], edge_in_ref.at[pl.ds(a, n)]) for a, n in ((0, 3), (3, 1), (4, 1), (5, 3), (8, 1), (9, 1))]
    views.append((collided_ref.at[pl.ds(0, 5)], x_low_ref))
    views.append((collided_ref.at[pl.ds(5, 5)], x_high_ref))
    return [
        pltpu.make_async_remote_copy(
            src_ref=source,
            dst_ref=target,
            send_sem=send_sem.at[n],
            recv_sem=recv_sem.at[n],
            **routed(ids[n]),
        )
        for n, (source, target) in enumerate(views)
    ]


def send_slip(refs):
    (cell_ref, mcount_ref, pcount_ref, pid_ref, table_ref, velocity_ref, pops_ref,
     flow_ref, cols_ref, slip_ref, wide_ref, pick_ref, message_ref) = refs
    width = cell_ref.shape[1]
    slabs = message_ref.shape[0]
    pick, spots = routes(pid_ref, table_ref, pcount_ref, width)
    pick_ref[...] = pick
    flow_table(pops_ref, flow_ref)
    slot_columns(velocity_ref, mcount_ref, pcount_ref, cols_ref)
    sample(cell_ref, flow_ref, cols_ref, slip_ref)
    slip = jnp.concatenate([slip_ref[c].astype(BF16) for c in range(3)], axis=1)
    put_rows(wide_ref, dot(pick_ref[...], slip), width)
    for p in range(2):
        wide_ref[pl.ds(6 + p, slabs, stride=8), :] = spots[p * slabs : (p + 1) * slabs]
    message_ref[...] = wide_ref[...].reshape(slabs, 8, width).astype(BF16)


def lubricate(got_ref, partner_ref, gap_ref, self_ref, pair_ref, reply_ref, wide_ref):
    slabs, _, width = got_ref.shape
    slots = 2 * slabs
    wide_ref[...] = got_ref[...].astype(F32).reshape(8 * slabs, width)
    owned = take_rows(wide_ref)
    spot_col = jnp.concatenate(
        [wide_ref[pl.ds(6 + p, slabs, stride=8), :] for p in range(2)], axis=0
    )
    head = ones_at(iota((slots, width), 1) == 0)
    spot_row = dot(head, spot_col.astype(BF16), NT)
    pairs = jnp.concatenate([partner_ref[...].astype(F32), gap_ref[...]], axis=0).T
    weight = jnp.zeros((slots, slots), F32)
    for k in range(4):
        weight += jnp.where(pairs[:, k : k + 1] + 1.0 == spot_row, 1.0 / pairs[:, 4 + k : 5 + k], 0.0)
    high, low = split_two(weight)
    near = (dot(high, owned) + dot(low, owned)).astype(BF16)
    place = ones_at(spot_col[:, :1] - 1.0 == iota((slots, slots), 1).astype(F32))
    near = dot(place, near).astype(BF16)
    parts = []
    for c in range(3):
        side = slice(c * width, (c + 1) * width)
        parts.append(dot(owned[:, side], self_ref[...]) + dot(near[:, side], pair_ref[...]))
    put_rows(wide_ref, jnp.concatenate(parts, axis=1), width)
    reply_ref[...] = wide_ref[...].reshape(slabs, 8, width).astype(BF16)


def spread(cell_ref, force_ref, rows, depth):
    slots, width = cell_ref.shape
    high_iota = iota((16, width), 0).astype(F32).astype(BF16)

    def block(g, total):
        at = pl.multiple_of(g * 8, 8)
        cell = cell_ref[pl.ds(at, 8), :]
        zf, yf = (part.astype(F32) for part in split_cell(cell, depth))
        vals = [force_ref[c, pl.ds(at, 8), :] for c in range(3)]

        def packed(value, j):
            return jnp.broadcast_to(value[j : j + 1, :], (16, width)).astype(BF16)

        for pair in range(4):
            a_side, b_side = [], []
            for j in (2 * pair, 2 * pair + 1):
                zb, yb = packed(zf, j), packed(yf, j)
                one, zero = jnp.ones((16, width), BF16), jnp.zeros((16, width), BF16)
                b_side.append(
                    jnp.concatenate(
                        [jnp.where(zb == high_iota + 16 * i, one, zero) for i in range(depth // 16)], axis=0
                    )
                )
                marks = [yb == high_iota + 16 * i for i in range(rows // 16)]
                lines = []
                for c in range(3):
                    vb = packed(vals[c], j)
                    lines += [jnp.where(mark, vb, zero) for mark in marks]
                a_side.append(jnp.concatenate(lines, axis=0))
            total = total + dot(jnp.concatenate(a_side, axis=1), jnp.concatenate(b_side, axis=1), NT)
        return total

    return lax.fori_loop(0, slots // 8, block, jnp.zeros((3 * rows, depth), F32))


def along(i, parts):
    terms = [parts[c] if DIRS[i][c] == 1 else -parts[c] for c in range(3) if DIRS[i][c] != 0]
    return functools.reduce(lambda a, b: a + b, terms) if terms else None


def collide(pops_ref, force, out_ref, chosen):
    density, moment = moments(pops_ref)
    inverse = 1.0 / density
    velocity = [(moment[c] + 0.5 * force[c]) * inverse for c in range(3)]
    speed_sq = velocity[0] * velocity[0] + velocity[1] * velocity[1] + velocity[2] * velocity[2]
    work = velocity[0] * force[0] + velocity[1] * force[1] + velocity[2] * force[2]
    base = 1.0 - 1.5 * speed_sq
    for i in chosen:
        w = WEIGHTS[i]
        cu, cf = along(i, velocity), along(i, force)
        if cu is None:
            equilibrium = w * density * base
            source = (1.0 - 0.5 * OMEGA) * w * (-3.0 * work)
        else:
            equilibrium = w * density * (base + 3.0 * cu + 4.5 * cu * cu)
            source = (1.0 - 0.5 * OMEGA) * w * (3.0 * (cf - work) + 9.0 * cu * cf)
        pops = pops_ref[i]
        out_ref[PLACE[i]] = pops - OMEGA * (pops - equilibrium) + source


def stream(chosen, collided_ref, x_low_ref, x_high_ref, edge_ref, read_ref):
    rows, depth = collided_ref.shape[1:]
    me = lax.axis_index("sub")
    last = lax.axis_size("sub") - 1
    row = iota((rows, depth), 0)
    for i in chosen:
        sx, sy, sz = DIRS[i]
        if sx == 0:
            value = collided_ref[PLACE[i]]
        elif sx == 1:
            value = x_low_ref[X_UP.index(i)]
        else:
            value = x_high_ref[X_DOWN.index(i)]
        if sy == 1:
            value = jnp.where(row == 0, edge_ref[EDGES.index(i)], pltpu.roll(value, 1, 0))
        elif sy == -1:
            value = jnp.where(row == rows - 1, edge_ref[EDGES.index(i)], pltpu.roll(value, rows - 1, 0))
        if sz != 0:
            value = pltpu.roll(value, sz % depth, 1)
        if sy != 0:
            wall_row, wall_device = (0, 0) if sy == 1 else (rows - 1, last)
            at_wall = (row == wall_row) & (me == wall_device)
            value = jnp.where(at_wall, collided_ref[PLACE[OPPOSITE[i]]], value)
        read_ref[i] = value


def step_kernel(
    pops_ref, cell_ref, mcount_ref, pcount_ref, pid_ref, table_ref, velocity_ref,
    partner_ref, gap_ref, self_ref, pair_ref,
    read_ref, marker_ref,
    flow_ref, cols_ref, slip_ref, wide_ref, pick_ref, message_ref, got_ref, reply_ref, returned_ref,
    collided_ref, x_low_ref, x_high_ref, edge_out_ref, edge_in_ref,
    bulk_sem, own_sem, halo_send, halo_recv,
):
    slots, width = cell_ref.shape
    rows, depth = pops_ref.shape[1:]
    greet()
    send_slip((cell_ref, mcount_ref, pcount_ref, pid_ref, table_ref, velocity_ref, pops_ref,
               flow_ref, cols_ref, slip_ref, wide_ref, pick_ref, message_ref))
    met()
    there = (message_ref, got_ref, bulk_sem.at[0], bulk_sem.at[1], own_sem.at[0])
    exchange_start(*there)
    exchange_wait(*there)
    lubricate(got_ref, partner_ref, gap_ref, self_ref, pair_ref, reply_ref, wide_ref)
    back = (reply_ref, returned_ref, bulk_sem.at[2], bulk_sem.at[3], own_sem.at[1])
    exchange_start(*back)
    exchange_wait(*back)
    wide_ref[...] = returned_ref[...].astype(F32).reshape(wide_ref.shape)
    own = dot(pick_ref[...], take_rows(wide_ref), TN)
    live = iota((slots, width), 1).astype(F32) < cols_ref[:, 3:4]
    for c in range(3):
        value = jnp.where(live, own[:, c * width : (c + 1) * width], 0.0)
        slip_ref[c] = value
        marker_ref[c] = value.astype(BF16)
    total = spread(cell_ref, slip_ref, rows, depth)
    force = [total[c * rows : (c + 1) * rows] for c in range(3)]
    collide(pops_ref, force, collided_ref, ORDER)
    for n, i in enumerate(EDGES):
        at = rows - 1 if DIRS[i][1] == 1 else 0
        edge_out_ref[n] = collided_ref[PLACE[i], at : at + 1, :]
    copies = halo_copies(collided_ref, x_low_ref, x_high_ref, edge_out_ref, edge_in_ref, halo_send, halo_recv)
    for copy in copies:
        copy.start()
    streams = (collided_ref, x_low_ref, x_high_ref, edge_in_ref, read_ref)
    inner = [0, 5, 6]
    stream(inner, *streams)
    for copy in copies:
        copy.wait()
    stream([i for i in range(19) if i not in inner], *streams)


def per_device(
    populations, marker_cell, marker_count, particle_count, particle_id, owner_table,
    particle_velocity, pair_list, pair_gap, self_coupling, pair_coupling,
):
    rows, depth = populations.shape[2:]
    slots, width = marker_cell.shape[2:]
    slabs = lax.axis_size("slab")
    args = (
        populations[:, 0],
        marker_cell[0, 0],
        marker_count[0],
        particle_count,
        particle_id[0],
        owner_table,
        jnp.transpose(particle_velocity[0], (1, 0, 2)),
        jnp.transpose(pair_list[0, 0]),
        jnp.transpose(pair_gap[0, 0]),
        self_coupling,
        pair_coupling,
    )
    place = pl.BlockSpec(memory_space=pltpu.VMEM)
    post = ((slabs, 8, width), BF16)
    scratch = [
        ((3 * rows, depth), F32),
        ((slots, 8), F32),
        ((3, slots, width), F32),
        ((8 * slabs, width), F32),
        ((slots, slots), BF16),
        post,
        post,
        post,
        post,
        ((19, rows, depth), F32),
        ((5, rows, depth), F32),
        ((5, rows, depth), F32),
        ((10, 1, depth), F32),
        ((10, 1, depth), F32),
    ]
    read, marker = pl.pallas_call(
        step_kernel,
        out_shape=[
            jax.ShapeDtypeStruct((19, rows, depth), F32),
            jax.ShapeDtypeStruct((3, slots, width), BF16),
        ],
        in_specs=[place] * len(args),
        out_specs=[place] * 2,
        scratch_shapes=[pltpu.VMEM(shape, kind) for shape, kind in scratch]
        + [
            pltpu.SemaphoreType.DMA((4,)),
            pltpu.SemaphoreType.DMA((2,)),
            pltpu.SemaphoreType.DMA((8,)),
            pltpu.SemaphoreType.DMA((8,)),
        ],
        compiler_params=pltpu.CompilerParams(collective_id=0, has_side_effects=True),
        name="step",
    )(*args)
    return read[:, None], jnp.transpose(marker, (1, 0, 2))[None, None]


def solution(mesh):
    placed = (
        P(None, "slab", "sub", None),
        P("slab", "sub", None, None),
        P("slab", "sub", None),
        P("slab", "sub"),
        P("slab", "sub", None),
        P("sub", None),
        P("slab", "sub", None, None),
        P("slab", "sub", None, None),
        P("slab", "sub", None, None),
        P(),
        P(),
    )
    return jax.shard_map(
        per_device,
        mesh=mesh,
        in_specs=placed,
        out_specs=(P(None, "slab", "sub", None), P("slab", "sub", None, None, None)),
        check_vma=False,
    )
```

```python
import functools

import jax
import jax.numpy as jnp
from jax import lax
from jax.experimental import pallas as pl
from jax.experimental.pallas import tpu as pltpu
from jax.sharding import PartitionSpec as P

DIRS = [
    (0, 0, 0),
    (1, 0, 0),
    (-1, 0, 0),
    (0, 1, 0),
    (0, -1, 0),
    (0, 0, 1),
    (0, 0, -1),
    (1, 1, 0),
    (-1, -1, 0),
    (1, -1, 0),
    (-1, 1, 0),
    (1, 0, 1),
    (-1, 0, -1),
    (1, 0, -1),
    (-1, 0, 1),
    (0, 1, 1),
    (0, -1, -1),
    (0, 1, -1),
    (0, -1, 1),
]
WEIGHTS = [1.0 / 3.0] + [1.0 / 18.0] * 6 + [1.0 / 36.0] * 12
OPPOSITE = [0, 2, 1, 4, 3, 6, 5, 8, 7, 10, 9, 12, 11, 14, 13, 16, 15, 18, 17]
OMEGA = 1.25
SAMPLE_GROUP = 8
SPREAD_GROUP = 16
FIXED = float(1 << 21)
VMEM_LIMIT = 60 * 1024 * 1024
X_UP = [i for i in range(19) if DIRS[i][0] == 1]
X_DOWN = [i for i in range(19) if DIRS[i][0] == -1]
Y_UP = [i for i in range(19) if DIRS[i][1] == 1]
Y_DOWN = [i for i in range(19) if DIRS[i][1] == -1]

F32 = jnp.float32
BF16 = jnp.bfloat16
NN = (((1,), (0,)), ((), ()))
NT = (((1,), (1,)), ((), ()))
TN = (((0,), (0,)), ((), ()))


def dot(a, b, dims=NN):
    return lax.dot_general(a, b, dims, preferred_element_type=F32)


def iota(shape, axis):
    return lax.broadcasted_iota(jnp.int32, shape, axis)


def ones_at(mask):
    return jnp.where(mask, 1.0, 0.0).astype(BF16)


def split_cell(cell, depth):
    return cell & (depth - 1), lax.shift_right_logical(cell, depth.bit_length() - 1)


def split_two(value):
    high = value.astype(BF16)
    return high, (value - high.astype(F32)).astype(BF16)


def moments(pops_ref):
    pops = [pops_ref[i] for i in range(19)]
    density = functools.reduce(lambda a, b: a + b, pops)
    moment = []
    for c in range(3):
        up = functools.reduce(lambda a, b: a + b, [pops[i] for i in range(19) if DIRS[i][c] == 1])
        down = functools.reduce(lambda a, b: a + b, [pops[i] for i in range(19) if DIRS[i][c] == -1])
        moment.append(up - down)
    return density, moment


def flow_table(pops_ref, flow_ref):
    rows = pops_ref.shape[1]
    density, moment = moments(pops_ref)
    x, y, z = ((moment[c] / density * FIXED + 0.5 * FIXED + 0.5).astype(jnp.int32) for c in range(3))
    high = lax.shift_right_logical(z, 10)
    flow_ref[pl.ds(0, rows), :] = lax.shift_left(x, 11) + high
    flow_ref[pl.ds(rows, rows), :] = lax.shift_left(y, 11) + (z & 1023)


def unpack_flow(first, second):
    x = lax.shift_right_logical(first, 11)
    y = lax.shift_right_logical(second, 11)
    z = lax.shift_left(first & 2047, 10) + (second & 2047)
    return [value.astype(F32) * (1.0 / FIXED) - 0.5 for value in (x, y, z)]


def slot_columns(velocity_ref, mcount_ref, pcount_ref, cols_ref):
    slots = mcount_ref.shape[1]
    lim = jnp.where(iota((1, slots), 1) < pcount_ref[...], mcount_ref[...], 0).astype(F32)
    stack = [velocity_ref[...].reshape(3, slots)] if velocity_ref is not None else [jnp.zeros((3, slots), F32)]
    stack = jnp.concatenate(stack + [lim, jnp.zeros((4, slots), F32)], axis=0)
    cols_ref[...] = stack.T


def routes(pid_ref, table_ref, pcount_ref, width):
    slots, slabs = pid_ref.shape[1], table_ref.shape[1]
    ids = pid_ref[...]
    alive = iota((1, slots), 1) < pcount_ref[...]
    in_range = ones_at(iota((slabs, slots), 0) == ids // slots)
    owner_of = ones_at(iota((slabs, slabs), 0) == table_ref[...])
    owner = jnp.where(alive, dot(owner_of, in_range), 0.0)
    before = ones_at(iota((slots, slots), 0) < iota((slots, slots), 1))
    earlier = dot(owner.astype(BF16), before)
    first = jnp.where(earlier < 0.5, owner, 0.0)
    pick = jnp.concatenate([first, owner - first], axis=0).astype(BF16)
    spot = (ids % slots + 1).astype(F32)
    spots = dot(pick, jnp.broadcast_to(spot, (width, slots)).astype(BF16), NT)
    return pick, spots


def sample(cell_ref, flow_ref, cols_ref, slip_ref, half):
    slots, width = cell_ref.shape
    rows = flow_ref.shape[0] // 2
    depth = flow_ref.shape[1]
    group = min(SAMPLE_GROUP, slots // 8)

    def block(g, carry):
        for n in range(group):
            at = pl.multiple_of(g * 8 * group + 8 * n, 8)
            z, y = split_cell(cell_ref[pl.ds(at, 8), :], depth)
            picked = [jnp.zeros((8, width), jnp.int32) for _ in range(2)]
            for row in range(rows):
                here = y == row
                for c in range(2):
                    line = jnp.broadcast_to(flow_ref[c * rows + row : c * rows + row + 1, :], (8, depth))
                    got = jnp.take_along_axis(line, z, axis=1, mode="promise_in_bounds")
                    picked[c] = jnp.where(here, got, picked[c])
            cols = cols_ref[pl.ds(at, 8), :]
            flow = unpack_flow(*picked)
            live = iota((8, width), 1).astype(F32) < cols[:, 3:4]
            for c in range(3):
                slip_ref[c, pl.ds(at, 8), :] = jnp.where(live, cols[:, c : c + 1] - flow[c], 0.0)
        return carry

    steps = slots // (8 * group)
    middle = steps // 2
    lax.fori_loop(middle if half else 0, steps if half else middle, block, 0)


def put_rows(wide_ref, rows, width):
    slabs = wide_ref.shape[0] // 8
    for p in range(2):
        for c in range(3):
            wide_ref[pl.ds(p * 3 + c, slabs, stride=8), :] = rows[
                p * slabs : (p + 1) * slabs, c * width : (c + 1) * width
            ]


def take_rows(wide_ref):
    slabs = wide_ref.shape[0] // 8
    sides = []
    for p in range(2):
        sides.append(
            jnp.concatenate(
                [wide_ref[pl.ds(p * 3 + c, slabs, stride=8), :] for c in range(3)], axis=1
            )
        )
    return jnp.concatenate(sides, axis=0).astype(BF16)


ORDER = X_UP + X_DOWN + [3, 4, 15, 16, 17, 18, 0, 5, 6]
PLACE = [ORDER.index(i) for i in range(19)]
EDGES = [3, 15, 17, 7, 10, 4, 16, 18, 9, 8]


def routed(mesh_ids):
    return dict(device_id=mesh_ids, device_id_type=pl.DeviceIdType.MESH)


def near_ids():
    slabs, subs = lax.axis_size("slab"), lax.axis_size("sub")
    me, side = lax.axis_index("slab"), lax.axis_index("sub")
    next_slab, last_slab = lax.rem(me + 1, slabs), lax.rem(me + slabs - 1, slabs)
    next_sub, last_sub = lax.rem(side + 1, subs), lax.rem(side + subs - 1, subs)
    return [
        {"slab": me, "sub": next_sub},
        {"slab": next_slab, "sub": next_sub},
        {"slab": last_slab, "sub": next_sub},
        {"slab": me, "sub": last_sub},
        {"slab": next_slab, "sub": last_sub},
        {"slab": last_slab, "sub": last_sub},
        {"slab": next_slab, "sub": side},
        {"slab": last_slab, "sub": side},
    ]


def inner_size():
    return 16 if lax.axis_size("slab") % 32 == 0 else 4


def greet():
    side = lax.axis_index("sub")
    barrier = pltpu.get_barrier_semaphore()
    for to in row_peers() + column_peers():
        pl.semaphore_signal(barrier, inc=1, **routed({"slab": to, "sub": side}))
    for ids in near_ids()[:6]:
        pl.semaphore_signal(barrier, inc=1, **routed(ids))


def row_peers():
    inner, me = inner_size(), lax.axis_index("slab")
    base = me // inner * inner
    return [base + lax.rem(me + k, inner) for k in range(1, inner)]


def column_peers():
    slabs, inner, me = lax.axis_size("slab"), inner_size(), lax.axis_index("slab")
    return [lax.rem(me + k * inner, slabs) for k in range(1, slabs // inner)]


def relay(row_sem):
    side = lax.axis_index("sub")
    rows, columns = row_peers(), column_peers()
    pl.semaphore_wait(pltpu.get_barrier_semaphore(), len(rows) + len(columns) + 6)
    for to in columns:
        pl.semaphore_signal(row_sem, inc=1, **routed({"slab": to, "sub": side}))


def met(row_sem):
    pl.semaphore_wait(row_sem, len(column_peers()))


def far_first(size):
    return sorted(range(size), key=lambda step: -min(step, size - step))


def exchange_start(out_ref, in_ref, send_sem, recv_sem, own_sem, lines):
    slabs, inner = lax.axis_size("slab"), inner_size()
    outer, ring = slabs // inner, inner // 2
    me, side = lax.axis_index("slab"), lax.axis_index("sub")
    bases = [lax.rem(me // inner + step, outer) * inner for step in far_first(outer)]
    place = lax.rem(me, inner) // 2
    cores = [lax.rem(me + 1, 2), lax.rem(me, 2)]

    def send(to):
        pltpu.make_async_remote_copy(
            src_ref=out_ref.at[to, pl.ds(0, lines)],
            dst_ref=in_ref.at[me, pl.ds(0, lines)],
            send_sem=send_sem,
            recv_sem=recv_sem,
            **routed({"slab": to, "sub": side}),
        ).start()

    def one(j, carry):
        step = ring // 2 + (j + 1) // 2 * (1 - 2 * lax.rem(j + 1, 2))
        here = lax.rem(place + step, ring) * 2
        for base in bases:
            for core in cores:
                send(base + here + core)
        return carry

    lax.fori_loop(0, ring - 1, one, 0)
    for base in bases[:-1]:
        for core in cores:
            send(base + place * 2 + core)
    send(bases[-1] + place * 2 + cores[0])
    pltpu.make_async_copy(out_ref.at[me], in_ref.at[me], own_sem).start()


def exchange_wait(out_ref, in_ref, send_sem, recv_sem, own_sem, lines):
    slabs = lax.axis_size("slab")
    me = lax.axis_index("slab")
    others = pl.ds(0, slabs - 1)
    pltpu.make_async_copy(out_ref.at[me], in_ref.at[me], own_sem).wait()
    pltpu.make_async_copy(in_ref.at[others, pl.ds(0, lines)], in_ref.at[others, pl.ds(0, lines)], recv_sem).wait()
    pltpu.make_async_copy(out_ref.at[others, pl.ds(0, lines)], out_ref.at[others, pl.ds(0, lines)], send_sem).wait()


def halo_copies(collided_ref, x_low_ref, x_high_ref, edge_out_ref, edge_in_ref, send_sem, recv_sem):
    ids = near_ids()
    views = [(edge_out_ref.at[pl.ds(a, n)], edge_in_ref.at[pl.ds(a, n)]) for a, n in ((0, 3), (3, 1), (4, 1), (5, 3), (8, 1), (9, 1))]
    views.append((collided_ref.at[pl.ds(0, 5)], x_low_ref))
    views.append((collided_ref.at[pl.ds(5, 5)], x_high_ref))
    return [
        pltpu.make_async_remote_copy(
            src_ref=source,
            dst_ref=target,
            send_sem=send_sem.at[n],
            recv_sem=recv_sem.at[n],
            **routed(ids[n]),
        )
        for n, (source, target) in enumerate(views)
    ]


def scope(name):
    return jax.named_scope(name)


def send_slip(refs):
    (cell_ref, mcount_ref, pcount_ref, pid_ref, table_ref, velocity_ref, pops_ref,
     flow_ref, cols_ref, slip_ref, wide_ref, pick_ref, message_ref, row_sem) = refs
    width = cell_ref.shape[1]
    slabs = message_ref.shape[0]
    with scope("q1_routes"):
        pick, spots = routes(pid_ref, table_ref, pcount_ref, width)
        pick_ref[...] = pick
        for p in range(2):
            wide_ref[pl.ds(6 + p, slabs, stride=8), :] = spots[p * slabs : (p + 1) * slabs]
    with scope("q2_flow"):
        flow_table(pops_ref, flow_ref)
    with scope("q3_cols"):
        slot_columns(velocity_ref, mcount_ref, pcount_ref, cols_ref)
    with scope("q4_sample"):
        sample(cell_ref, flow_ref, cols_ref, slip_ref, 0)
    with scope("q5_relay"):
        relay(row_sem)
    with scope("q6_sample"):
        sample(cell_ref, flow_ref, cols_ref, slip_ref, 1)
    slip = jnp.concatenate([slip_ref[c].astype(BF16) for c in range(3)], axis=1)
    put_rows(wide_ref, dot(pick_ref[...], slip), width)
    message_ref[...] = wide_ref[...].reshape(slabs, 8, width).astype(BF16)


def pair_columns(partner_ref, gap_ref, pairs_ref):
    pairs_ref[...] = jnp.concatenate([partner_ref[...].astype(F32) + 1.0, 1.0 / gap_ref[...]], axis=0).T


def lubricate(got_ref, pairs_ref, self_ref, pair_ref, reply_ref, wide_ref):
    slabs, _, width = got_ref.shape
    slots = 2 * slabs
    wide_ref[...] = got_ref[...].astype(F32).reshape(8 * slabs, width)
    owned = take_rows(wide_ref)
    spot_col = jnp.concatenate(
        [wide_ref[pl.ds(6 + p, slabs, stride=8), :] for p in range(2)], axis=0
    )
    head = ones_at(iota((slots, width), 1) == 0)
    spot_row = dot(head, spot_col.astype(BF16), NT)
    pairs = pairs_ref[...]
    weight = jnp.zeros((slots, slots), F32)
    for k in range(4):
        weight += jnp.where(pairs[:, k : k + 1] == spot_row, pairs[:, 4 + k : 5 + k], 0.0)
    high, low = split_two(weight)
    near = (dot(high, owned) + dot(low, owned)).astype(BF16)
    place = ones_at(spot_col[:, :1] - 1.0 == iota((slots, slots), 1).astype(F32))
    near = dot(place, near).astype(BF16)
    parts = []
    for c in range(3):
        side = slice(c * width, (c + 1) * width)
        parts.append(dot(owned[:, side], self_ref[...]) + dot(near[:, side], pair_ref[...]))
    put_rows(wide_ref, jnp.concatenate(parts, axis=1), width)
    reply_ref[...] = wide_ref[...].reshape(slabs, 8, width).astype(BF16)


def packed_row(value, j):
    return jnp.broadcast_to(value[j : j + 1, :], (16, value.shape[1])).astype(BF16)


def mark_depths(cell_ref, hot_ref, depth):
    slots, width = cell_ref.shape
    lines = iota((16, width), 0).astype(F32).astype(BF16)
    one, zero = jnp.ones((16, width), BF16), jnp.zeros((16, width), BF16)

    def block(g, carry):
        z = split_cell(cell_ref[pl.ds(pl.multiple_of(g * 8, 8), 8), :], depth)[0].astype(F32)
        for j in range(8):
            zb = packed_row(z, j)
            for i in range(depth // 16):
                hot_ref[g, 16 * i : 16 * (i + 1), j * width : (j + 1) * width] = jnp.where(
                    zb == lines + 16 * i, one, zero
                )
        return carry

    lax.fori_loop(0, slots // 8, block, 0)


def spread(cell_ref, force_ref, hot_ref, rows, depth):
    slots, width = cell_ref.shape
    lines = iota((16, width), 0).astype(F32).astype(BF16)
    zero = jnp.zeros((16, width), BF16)

    group = min(SPREAD_GROUP, slots // 8)

    def block(g, total):
        for n in range(group):
            at = pl.multiple_of(g * 8 * group + 8 * n, 8)
            y = split_cell(cell_ref[pl.ds(at, 8), :], depth)[1].astype(F32)
            vals = [force_ref[c, pl.ds(at, 8), :] for c in range(3)]
            sides = []
            for j in range(8):
                yb = packed_row(y, j)
                marks = [yb == lines + 16 * i for i in range(rows // 16)]
                stack = []
                for c in range(3):
                    vb = packed_row(vals[c], j)
                    stack += [jnp.where(mark, vb, zero) for mark in marks]
                sides.append(jnp.concatenate(stack, axis=0))
            total = total + dot(jnp.concatenate(sides, axis=1), hot_ref[g * group + n], NT)
        return total

    return lax.fori_loop(0, slots // (8 * group), block, jnp.zeros((3 * rows, depth), F32))


def along(i, parts):
    terms = [parts[c] if DIRS[i][c] == 1 else -parts[c] for c in range(3) if DIRS[i][c] != 0]
    return functools.reduce(lambda a, b: a + b, terms) if terms else None


def collide(pops_ref, force, out_ref, chosen):
    density, moment = moments(pops_ref)
    inverse = 1.0 / density
    velocity = [(moment[c] + 0.5 * force[c]) * inverse for c in range(3)]
    speed_sq = velocity[0] * velocity[0] + velocity[1] * velocity[1] + velocity[2] * velocity[2]
    work = velocity[0] * force[0] + velocity[1] * force[1] + velocity[2] * force[2]
    base = 1.0 - 1.5 * speed_sq
    for i in chosen:
        w = WEIGHTS[i]
        cu, cf = along(i, velocity), along(i, force)
        if cu is None:
            equilibrium = w * density * base
            source = (1.0 - 0.5 * OMEGA) * w * (-3.0 * work)
        else:
            equilibrium = w * density * (base + 3.0 * cu + 4.5 * cu * cu)
            source = (1.0 - 0.5 * OMEGA) * w * (3.0 * (cf - work) + 9.0 * cu * cf)
        pops = pops_ref[i]
        out_ref[PLACE[i]] = pops - OMEGA * (pops - equilibrium) + source


def stream(chosen, collided_ref, x_low_ref, x_high_ref, edge_ref, read_ref):
    rows, depth = collided_ref.shape[1:]
    me = lax.axis_index("sub")
    last = lax.axis_size("sub") - 1
    row = iota((rows, depth), 0)
    for i in chosen:
        sx, sy, sz = DIRS[i]
        if sx == 0:
            value = collided_ref[PLACE[i]]
        elif sx == 1:
            value = x_low_ref[X_UP.index(i)]
        else:
            value = x_high_ref[X_DOWN.index(i)]
        if sy == 1:
            value = jnp.where(row == 0, edge_ref[EDGES.index(i)], pltpu.roll(value, 1, 0))
        elif sy == -1:
            value = jnp.where(row == rows - 1, edge_ref[EDGES.index(i)], pltpu.roll(value, rows - 1, 0))
        if sz != 0:
            value = pltpu.roll(value, sz % depth, 1)
        if sy != 0:
            wall_row, wall_device = (0, 0) if sy == 1 else (rows - 1, last)
            at_wall = (row == wall_row) & (me == wall_device)
            value = jnp.where(at_wall, collided_ref[PLACE[OPPOSITE[i]]], value)
        read_ref[i] = value


def step_kernel(*refs):
    given, (read_ref, marker_ref), rest = refs[:11], refs[11:13], refs[13:]
    held, rest = rest[:11], rest[11:]
    (pops_ref, cell_ref, mcount_ref, pcount_ref, pid_ref, table_ref, velocity_ref,
     partner_ref, gap_ref, self_ref, pair_ref) = held
    (flow_ref, cols_ref, slip_ref, wide_ref, pick_ref, message_ref, got_ref, reply_ref, returned_ref,
     collided_ref, x_low_ref, x_high_ref, edge_out_ref, edge_in_ref, hot_ref, pairs_ref,
     load_sem, bulk_sem, own_sem, halo_send, halo_recv, row_sem) = rest
    slots, width = cell_ref.shape
    rows, depth = pops_ref.shape[1:]
    loads = [pltpu.make_async_copy(a, b, load_sem.at[n]) for n, (a, b) in enumerate(zip(given, held))]
    for load in loads:
        load.start()
    with scope("p0_greet"):
        greet()
    with scope("p0_load"):
        for load in loads:
            load.wait()
    with scope("p1_front"):
        send_slip((cell_ref, mcount_ref, pcount_ref, pid_ref, table_ref, velocity_ref, pops_ref,
                   flow_ref, cols_ref, slip_ref, wide_ref, pick_ref, message_ref, row_sem))
    with scope("p2_met"):
        met(row_sem)
    there = (message_ref, got_ref, bulk_sem.at[0], bulk_sem.at[1], own_sem.at[0], 8)
    with scope("p3_start"):
        exchange_start(*there)
    with scope("p3_mark"):
        pair_columns(partner_ref, gap_ref, pairs_ref)
        mark_depths(cell_ref, hot_ref, depth)
    with scope("p4_wait"):
        exchange_wait(*there)
    with scope("p5_lub"):
        lubricate(got_ref, pairs_ref, self_ref, pair_ref, reply_ref, wide_ref)
    back = (reply_ref, returned_ref, bulk_sem.at[2], bulk_sem.at[3], own_sem.at[1], 6)
    with scope("p6_start"):
        exchange_start(*back)
    with scope("p7_wait"):
        exchange_wait(*back)
    with scope("p8_unroute"):
        wide_ref[...] = returned_ref[...].astype(F32).reshape(wide_ref.shape)
        own = dot(pick_ref[...], take_rows(wide_ref), TN)
        live = iota((slots, width), 1).astype(F32) < cols_ref[:, 3:4]
        for c in range(3):
            value = jnp.where(live, own[:, c * width : (c + 1) * width], 0.0)
            slip_ref[c] = value
            marker_ref[c] = value.astype(BF16)
    with scope("p9_spread"):
        total = spread(cell_ref, slip_ref, hot_ref, rows, depth)
    with scope("pa_collide"):
        force = [total[c * rows : (c + 1) * rows] for c in range(3)]
        collide(pops_ref, force, collided_ref, ORDER)
        for n, i in enumerate(EDGES):
            at = rows - 1 if DIRS[i][1] == 1 else 0
            edge_out_ref[n] = collided_ref[PLACE[i], at : at + 1, :]
    copies = halo_copies(collided_ref, x_low_ref, x_high_ref, edge_out_ref, edge_in_ref, halo_send, halo_recv)
    for copy in copies:
        copy.start()
    streams = (collided_ref, x_low_ref, x_high_ref, edge_in_ref, read_ref)
    inner = [0, 5, 6]
    with scope("pc_inner"):
        stream(inner, *streams)
    with scope("pd_hwait"):
        for copy in copies:
            copy.wait()
    with scope("pe_stream"):
        stream([i for i in range(19) if i not in inner], *streams)


def per_device(
    populations, marker_cell, marker_count, particle_count, particle_id, owner_table,
    particle_velocity, pair_list, pair_gap, self_coupling, pair_coupling,
):
    rows, depth = populations.shape[2:]
    slots, width = marker_cell.shape[2:]
    slabs = lax.axis_size("slab")
    args = (
        populations[:, 0],
        marker_cell[0, 0],
        marker_count[0],
        particle_count,
        particle_id[0],
        owner_table,
        jnp.transpose(particle_velocity[0], (1, 0, 2)),
        jnp.transpose(pair_list[0, 0]),
        jnp.transpose(pair_gap[0, 0]),
        self_coupling,
        pair_coupling,
    )
    place = pl.BlockSpec(memory_space=pltpu.VMEM)
    post = ((slabs, 8, width), BF16)
    scratch = [
        ((2 * rows, depth), jnp.int32),
        ((slots, 8), F32),
        ((3, slots, width), F32),
        ((8 * slabs, width), F32),
        ((slots, slots), BF16),
        post,
        post,
        post,
        post,
        ((19, rows, depth), F32),
        ((5, rows, depth), F32),
        ((5, rows, depth), F32),
        ((10, 1, depth), F32),
        ((10, 1, depth), F32),
        ((slots // 8, depth, 8 * width), BF16),
        ((slots, 8), F32),
    ]
    held = [(arg.shape, arg.dtype) for arg in args]
    read, marker = pl.pallas_call(
        step_kernel,
        out_shape=[
            jax.ShapeDtypeStruct((19, rows, depth), F32),
            jax.ShapeDtypeStruct((3, slots, width), BF16),
        ],
        in_specs=[pl.BlockSpec(memory_space=pltpu.HBM)] * len(args),
        out_specs=[place] * 2,
        scratch_shapes=[pltpu.VMEM(shape, kind) for shape, kind in held + scratch]
        + [
            pltpu.SemaphoreType.DMA((len(args),)),
            pltpu.SemaphoreType.DMA((4,)),
            pltpu.SemaphoreType.DMA((2,)),
            pltpu.SemaphoreType.DMA((8,)),
            pltpu.SemaphoreType.DMA((8,)),
            pltpu.SemaphoreType.REGULAR,
        ],
        compiler_params=pltpu.CompilerParams(
            collective_id=0, has_side_effects=True, vmem_limit_bytes=VMEM_LIMIT
        ),
        name="step",
    )(*args)
    return read[:, None], jnp.transpose(marker, (1, 0, 2))[None, None]


def solution(mesh):
    placed = (
        P(None, "slab", "sub", None),
        P("slab", "sub", None, None),
        P("slab", "sub", None),
        P("slab", "sub"),
        P("slab", "sub", None),
        P("sub", None),
        P("slab", "sub", None, None),
        P("slab", "sub", None, None),
        P("slab", "sub", None, None),
        P(),
        P(),
    )
    return jax.shard_map(
        per_device,
        mesh=mesh,
        in_specs=placed,
        out_specs=(P(None, "slab", "sub", None), P("slab", "sub", None, None, None)),
        check_vma=False,
    )
```

```python
import functools

import jax
import jax.numpy as jnp
from jax import lax
from jax.experimental import pallas as pl
from jax.experimental.pallas import tpu as pltpu
from jax.sharding import PartitionSpec as P

DIRS = [
    (0, 0, 0),
    (1, 0, 0),
    (-1, 0, 0),
    (0, 1, 0),
    (0, -1, 0),
    (0, 0, 1),
    (0, 0, -1),
    (1, 1, 0),
    (-1, -1, 0),
    (1, -1, 0),
    (-1, 1, 0),
    (1, 0, 1),
    (-1, 0, -1),
    (1, 0, -1),
    (-1, 0, 1),
    (0, 1, 1),
    (0, -1, -1),
    (0, 1, -1),
    (0, -1, 1),
]
WEIGHTS = [1.0 / 3.0] + [1.0 / 18.0] * 6 + [1.0 / 36.0] * 12
OPPOSITE = [0, 2, 1, 4, 3, 6, 5, 8, 7, 10, 9, 12, 11, 14, 13, 16, 15, 18, 17]
OMEGA = 1.25
SAMPLE_GROUP = 8
SPREAD_GROUP = 16
FIXED = float(1 << 21)
VMEM_LIMIT = 32 * 1024 * 1024
X_UP = [i for i in range(19) if DIRS[i][0] == 1]
X_DOWN = [i for i in range(19) if DIRS[i][0] == -1]
Y_UP = [i for i in range(19) if DIRS[i][1] == 1]
Y_DOWN = [i for i in range(19) if DIRS[i][1] == -1]

F32 = jnp.float32
BF16 = jnp.bfloat16
NN = (((1,), (0,)), ((), ()))
NT = (((1,), (1,)), ((), ()))
TN = (((0,), (0,)), ((), ()))


def dot(a, b, dims=NN):
    return lax.dot_general(a, b, dims, preferred_element_type=F32)


def iota(shape, axis):
    return lax.broadcasted_iota(jnp.int32, shape, axis)


def ones_at(mask):
    return jnp.where(mask, 1.0, 0.0).astype(BF16)


def split_cell(cell, depth):
    return cell & (depth - 1), lax.shift_right_logical(cell, depth.bit_length() - 1)


def split_two(value):
    high = value.astype(BF16)
    return high, (value - high.astype(F32)).astype(BF16)


def moments(pops_ref):
    pops = [pops_ref[i] for i in range(19)]
    density = functools.reduce(lambda a, b: a + b, pops)
    moment = []
    for c in range(3):
        up = functools.reduce(lambda a, b: a + b, [pops[i] for i in range(19) if DIRS[i][c] == 1])
        down = functools.reduce(lambda a, b: a + b, [pops[i] for i in range(19) if DIRS[i][c] == -1])
        moment.append(up - down)
    return density, moment


def flow_table(pops_ref, flow_ref):
    rows = pops_ref.shape[1]
    density, moment = moments(pops_ref)
    x, y, z = ((moment[c] / density * FIXED + 0.5 * FIXED + 0.5).astype(jnp.int32) for c in range(3))
    high = lax.shift_right_logical(z, 10)
    flow_ref[pl.ds(0, rows), :] = lax.shift_left(x, 11) + high
    flow_ref[pl.ds(rows, rows), :] = lax.shift_left(y, 11) + (z & 1023)


def unpack_flow(first, second):
    x = lax.shift_right_logical(first, 11)
    y = lax.shift_right_logical(second, 11)
    z = lax.shift_left(first & 2047, 10) + (second & 2047)
    return [value.astype(F32) * (1.0 / FIXED) - 0.5 for value in (x, y, z)]


def slot_columns(velocity_ref, mcount_ref, pcount_ref, cols_ref):
    slots = mcount_ref.shape[1]
    lim = jnp.where(iota((1, slots), 1) < pcount_ref[...], mcount_ref[...], 0).astype(F32)
    stack = [velocity_ref[...].reshape(3, slots)] if velocity_ref is not None else [jnp.zeros((3, slots), F32)]
    stack = jnp.concatenate(stack + [lim, jnp.zeros((4, slots), F32)], axis=0)
    cols_ref[...] = stack.T


def routes(pid_ref, table_ref, pcount_ref, width):
    slots, slabs = pid_ref.shape[1], table_ref.shape[1]
    ids = pid_ref[...]
    alive = iota((1, slots), 1) < pcount_ref[...]
    in_range = ones_at(iota((slabs, slots), 0) == ids // slots)
    owner_of = ones_at(iota((slabs, slabs), 0) == table_ref[...])
    owner = jnp.where(alive, dot(owner_of, in_range), 0.0)
    before = ones_at(iota((slots, slots), 0) < iota((slots, slots), 1))
    earlier = dot(owner.astype(BF16), before)
    first = jnp.where(earlier < 0.5, owner, 0.0)
    pick = jnp.concatenate([first, owner - first], axis=0).astype(BF16)
    spot = (ids % slots + 1).astype(F32)
    spots = dot(pick, jnp.broadcast_to(spot, (width, slots)).astype(BF16), NT)
    return pick, spots


def sample(cell_ref, flow_ref, cols_ref, slip_ref, half):
    slots, width = cell_ref.shape
    rows = flow_ref.shape[0] // 2
    depth = flow_ref.shape[1]
    group = min(SAMPLE_GROUP, slots // 8)

    def block(g, carry):
        for n in range(group):
            at = pl.multiple_of(g * 8 * group + 8 * n, 8)
            z, y = split_cell(cell_ref[pl.ds(at, 8), :], depth)
            picked = [jnp.zeros((8, width), jnp.int32) for _ in range(2)]
            for row in range(rows):
                here = y == row
                for c in range(2):
                    line = jnp.broadcast_to(flow_ref[c * rows + row : c * rows + row + 1, :], (8, depth))
                    got = jnp.take_along_axis(line, z, axis=1, mode="promise_in_bounds")
                    picked[c] = jnp.where(here, got, picked[c])
            cols = cols_ref[pl.ds(at, 8), :]
            flow = unpack_flow(*picked)
            live = iota((8, width), 1).astype(F32) < cols[:, 3:4]
            for c in range(3):
                slip_ref[c, pl.ds(at, 8), :] = jnp.where(live, cols[:, c : c + 1] - flow[c], 0.0)
        return carry

    steps = slots // (8 * group)
    middle = steps // 2
    lax.fori_loop(middle if half else 0, steps if half else middle, block, 0)


def put_rows(wide_ref, rows, width):
    slabs = wide_ref.shape[0] // 8
    for p in range(2):
        for c in range(3):
            wide_ref[pl.ds(p * 3 + c, slabs, stride=8), :] = rows[
                p * slabs : (p + 1) * slabs, c * width : (c + 1) * width
            ]


def take_rows(wide_ref):
    slabs = wide_ref.shape[0] // 8
    sides = []
    for p in range(2):
        sides.append(
            jnp.concatenate(
                [wide_ref[pl.ds(p * 3 + c, slabs, stride=8), :] for c in range(3)], axis=1
            )
        )
    return jnp.concatenate(sides, axis=0).astype(BF16)


ORDER = X_UP + X_DOWN + [3, 4, 15, 16, 17, 18, 0, 5, 6]
PLACE = [ORDER.index(i) for i in range(19)]
EDGES = [3, 15, 17, 7, 10, 4, 16, 18, 9, 8]


def routed(mesh_ids):
    return dict(device_id=mesh_ids, device_id_type=pl.DeviceIdType.MESH)


def near_ids():
    slabs, subs = lax.axis_size("slab"), lax.axis_size("sub")
    me, side = lax.axis_index("slab"), lax.axis_index("sub")
    next_slab, last_slab = lax.rem(me + 1, slabs), lax.rem(me + slabs - 1, slabs)
    next_sub, last_sub = lax.rem(side + 1, subs), lax.rem(side + subs - 1, subs)
    return [
        {"slab": me, "sub": next_sub},
        {"slab": next_slab, "sub": next_sub},
        {"slab": last_slab, "sub": next_sub},
        {"slab": me, "sub": last_sub},
        {"slab": next_slab, "sub": last_sub},
        {"slab": last_slab, "sub": last_sub},
        {"slab": next_slab, "sub": side},
        {"slab": last_slab, "sub": side},
    ]


def inner_size():
    return 16 if lax.axis_size("slab") % 32 == 0 else 4


def neighbours():
    side = lax.axis_index("sub")
    return side < lax.axis_size("sub") - 1, side > 0


def greet():
    side = lax.axis_index("sub")
    barrier = pltpu.get_barrier_semaphore()
    for to in row_peers() + column_peers():
        pl.semaphore_signal(barrier, inc=1, **routed({"slab": to, "sub": side}))
    ids = near_ids()
    for beside, chosen in zip(neighbours(), (ids[0:3], ids[3:6])):

        @pl.when(beside)
        def _():
            for one in chosen:
                pl.semaphore_signal(barrier, inc=1, **routed(one))


def row_peers():
    inner, me = inner_size(), lax.axis_index("slab")
    base = me // inner * inner
    return [base + lax.rem(me + k, inner) for k in range(1, inner)]


def column_peers():
    slabs, inner, me = lax.axis_size("slab"), inner_size(), lax.axis_index("slab")
    return [lax.rem(me + k * inner, slabs) for k in range(1, slabs // inner)]


def relay(row_sem):
    side = lax.axis_index("sub")
    rows, columns = row_peers(), column_peers()
    last = lax.axis_size("sub") - 1
    beside = (side + last - 1) // last + (2 * last - 1 - side) // last
    pl.semaphore_wait(pltpu.get_barrier_semaphore(), len(rows) + len(columns) + 3 * beside)
    for to in columns:
        pl.semaphore_signal(row_sem, inc=1, **routed({"slab": to, "sub": side}))


def met(row_sem):
    pl.semaphore_wait(row_sem, len(column_peers()))


def far_first(size):
    return sorted(range(size), key=lambda step: -min(step, size - step))


def exchange_start(out_ref, in_ref, send_sem, recv_sem, own_sem, lines):
    slabs, inner = lax.axis_size("slab"), inner_size()
    outer, ring = slabs // inner, inner // 2
    me, side = lax.axis_index("slab"), lax.axis_index("sub")
    bases = [lax.rem(me // inner + step, outer) * inner for step in far_first(outer)]
    place = lax.rem(me, inner) // 2
    cores = [lax.rem(me + 1, 2), lax.rem(me, 2)]

    def send(to):
        pltpu.make_async_remote_copy(
            src_ref=out_ref.at[to, pl.ds(0, lines)],
            dst_ref=in_ref.at[me, pl.ds(0, lines)],
            send_sem=send_sem,
            recv_sem=recv_sem,
            **routed({"slab": to, "sub": side}),
        ).start()

    def one(j, carry):
        step = ring // 2 + (j + 1) // 2 * (1 - 2 * lax.rem(j + 1, 2))
        here = lax.rem(place + step, ring) * 2
        for base in bases:
            for core in cores:
                send(base + here + core)
        return carry

    lax.fori_loop(0, ring - 1, one, 0)
    for base in bases[:-1]:
        for core in cores:
            send(base + place * 2 + core)
    send(bases[-1] + place * 2 + cores[0])
    pltpu.make_async_copy(out_ref.at[me], in_ref.at[me], own_sem).start()


def exchange_wait(out_ref, in_ref, send_sem, recv_sem, own_sem, lines):
    slabs = lax.axis_size("slab")
    me = lax.axis_index("slab")
    others = pl.ds(0, slabs - 1)
    pltpu.make_async_copy(out_ref.at[me], in_ref.at[me], own_sem).wait()
    pltpu.make_async_copy(in_ref.at[others, pl.ds(0, lines)], in_ref.at[others, pl.ds(0, lines)], recv_sem).wait()
    pltpu.make_async_copy(out_ref.at[others, pl.ds(0, lines)], out_ref.at[others, pl.ds(0, lines)], send_sem).wait()


def halo_copies(collided_ref, x_low_ref, x_high_ref, edge_out_ref, edge_in_ref, send_sem, recv_sem):
    ids = near_ids()
    views = [(edge_out_ref.at[pl.ds(a, n)], edge_in_ref.at[pl.ds(a, n)]) for a, n in ((0, 3), (3, 1), (4, 1), (5, 3), (8, 1), (9, 1))]
    views.append((collided_ref.at[pl.ds(0, 5)], x_low_ref))
    views.append((collided_ref.at[pl.ds(5, 5)], x_high_ref))
    return [
        pltpu.make_async_remote_copy(
            src_ref=source,
            dst_ref=target,
            send_sem=send_sem.at[n],
            recv_sem=recv_sem.at[n],
            **routed(ids[n]),
        )
        for n, (source, target) in enumerate(views)
    ]


def scope(name):
    return jax.named_scope(name)


def send_slip(refs):
    (cell_ref, mcount_ref, pcount_ref, pid_ref, table_ref, velocity_ref, pops_ref,
     flow_ref, cols_ref, slip_ref, wide_ref, pick_ref, message_ref, row_sem) = refs
    width = cell_ref.shape[1]
    slabs = message_ref.shape[0]
    with scope("q1_routes"):
        pick, spots = routes(pid_ref, table_ref, pcount_ref, width)
        pick_ref[...] = pick
        for p in range(2):
            wide_ref[pl.ds(6 + p, slabs, stride=8), :] = spots[p * slabs : (p + 1) * slabs]
    with scope("q2_flow"):
        flow_table(pops_ref, flow_ref)
    with scope("q3_cols"):
        slot_columns(velocity_ref, mcount_ref, pcount_ref, cols_ref)
    with scope("q4_sample"):
        sample(cell_ref, flow_ref, cols_ref, slip_ref, 0)
    with scope("q5_relay"):
        relay(row_sem)
    with scope("q6_sample"):
        sample(cell_ref, flow_ref, cols_ref, slip_ref, 1)
    slip = jnp.concatenate([slip_ref[c].astype(BF16) for c in range(3)], axis=1)
    put_rows(wide_ref, dot(pick_ref[...], slip), width)
    message_ref[...] = wide_ref[...].reshape(slabs, 8, width).astype(BF16)


def pair_columns(partner_ref, gap_ref, pairs_ref):
    pairs_ref[...] = jnp.concatenate([partner_ref[...].astype(F32) + 1.0, 1.0 / gap_ref[...]], axis=0).T


def lubricate(got_ref, pairs_ref, self_ref, pair_ref, reply_ref, wide_ref):
    slabs, _, width = got_ref.shape
    slots = 2 * slabs
    wide_ref[...] = got_ref[...].astype(F32).reshape(8 * slabs, width)
    owned = take_rows(wide_ref)
    spot_col = jnp.concatenate(
        [wide_ref[pl.ds(6 + p, slabs, stride=8), :] for p in range(2)], axis=0
    )
    head = ones_at(iota((slots, width), 1) == 0)
    spot_row = dot(head, spot_col.astype(BF16), NT)
    pairs = pairs_ref[...]
    weight = jnp.zeros((slots, slots), F32)
    for k in range(4):
        weight += jnp.where(pairs[:, k : k + 1] == spot_row, pairs[:, 4 + k : 5 + k], 0.0)
    high, low = split_two(weight)
    near = (dot(high, owned) + dot(low, owned)).astype(BF16)
    place = ones_at(spot_col[:, :1] - 1.0 == iota((slots, slots), 1).astype(F32))
    near = dot(place, near).astype(BF16)
    parts = []
    for c in range(3):
        side = slice(c * width, (c + 1) * width)
        parts.append(dot(owned[:, side], self_ref[...]) + dot(near[:, side], pair_ref[...]))
    put_rows(wide_ref, jnp.concatenate(parts, axis=1), width)
    reply_ref[...] = wide_ref[...].reshape(slabs, 8, width).astype(BF16)


def packed_row(value, j):
    return jnp.broadcast_to(value[j : j + 1, :], (16, value.shape[1])).astype(BF16)


def mark_depths(cell_ref, hot_ref, depth, half):
    slots, width = cell_ref.shape
    lanes = iota((width, depth), 1).astype(F32)

    def block(g, carry):
        z = split_cell(cell_ref[pl.ds(pl.multiple_of(g * 8, 8), 8), :], depth)[0].astype(F32).T
        for j in range(8):
            hot_ref[g, j * width : (j + 1) * width, :] = ones_at(z[:, j : j + 1] == lanes)
        return carry

    steps = slots // 8
    middle = steps // 2
    lax.fori_loop(middle if half else 0, steps if half else middle, block, 0)


def spread(cell_ref, force_ref, hot_ref, rows, depth):
    slots, width = cell_ref.shape
    lines = iota((16, width), 0).astype(F32).astype(BF16)
    zero = jnp.zeros((16, width), BF16)

    group = min(SPREAD_GROUP, slots // 8)

    def block(g, total):
        for n in range(group):
            at = pl.multiple_of(g * 8 * group + 8 * n, 8)
            y = split_cell(cell_ref[pl.ds(at, 8), :], depth)[1].astype(F32)
            vals = [force_ref[c, pl.ds(at, 8), :] for c in range(3)]
            sides = []
            for j in range(8):
                yb = packed_row(y, j)
                marks = [yb == lines + 16 * i for i in range(rows // 16)]
                stack = []
                for c in range(3):
                    vb = packed_row(vals[c], j)
                    stack += [jnp.where(mark, vb, zero) for mark in marks]
                sides.append(jnp.concatenate(stack, axis=0))
            total = total + dot(jnp.concatenate(sides, axis=1), hot_ref[g * group + n])
        return total

    return lax.fori_loop(0, slots // (8 * group), block, jnp.zeros((3 * rows, depth), F32))


def along(i, parts):
    terms = [parts[c] if DIRS[i][c] == 1 else -parts[c] for c in range(3) if DIRS[i][c] != 0]
    return functools.reduce(lambda a, b: a + b, terms) if terms else None


def collide(pops_ref, force, out_ref, chosen):
    density, moment = moments(pops_ref)
    inverse = 1.0 / density
    velocity = [(moment[c] + 0.5 * force[c]) * inverse for c in range(3)]
    speed_sq = velocity[0] * velocity[0] + velocity[1] * velocity[1] + velocity[2] * velocity[2]
    work = velocity[0] * force[0] + velocity[1] * force[1] + velocity[2] * force[2]
    base = 1.0 - 1.5 * speed_sq
    for i in chosen:
        w = WEIGHTS[i]
        cu, cf = along(i, velocity), along(i, force)
        if cu is None:
            equilibrium = w * density * base
            source = (1.0 - 0.5 * OMEGA) * w * (-3.0 * work)
        else:
            equilibrium = w * density * (base + 3.0 * cu + 4.5 * cu * cu)
            source = (1.0 - 0.5 * OMEGA) * w * (3.0 * (cf - work) + 9.0 * cu * cf)
        pops = pops_ref[i]
        out_ref[PLACE[i]] = pops - OMEGA * (pops - equilibrium) + source


def stream(chosen, collided_ref, x_low_ref, x_high_ref, edge_ref, read_ref):
    rows, depth = collided_ref.shape[1:]
    me = lax.axis_index("sub")
    last = lax.axis_size("sub") - 1
    row = iota((rows, depth), 0)
    for i in chosen:
        sx, sy, sz = DIRS[i]
        if sx == 0:
            value = collided_ref[PLACE[i]]
        elif sx == 1:
            value = x_low_ref[X_UP.index(i)]
        else:
            value = x_high_ref[X_DOWN.index(i)]
        if sy == 1:
            value = jnp.where(row == 0, edge_ref[EDGES.index(i)], pltpu.roll(value, 1, 0))
        elif sy == -1:
            value = jnp.where(row == rows - 1, edge_ref[EDGES.index(i)], pltpu.roll(value, rows - 1, 0))
        if sz != 0:
            value = pltpu.roll(value, sz % depth, 1)
        if sy != 0:
            wall_row, wall_device = (0, 0) if sy == 1 else (rows - 1, last)
            at_wall = (row == wall_row) & (me == wall_device)
            value = jnp.where(at_wall, collided_ref[PLACE[OPPOSITE[i]]], value)
        read_ref[i] = value


def step_kernel(*refs):
    given, (read_ref, marker_ref), rest = refs[:11], refs[11:13], refs[13:]
    held, rest = rest[:11], rest[11:]
    (pops_ref, cell_ref, mcount_ref, pcount_ref, pid_ref, table_ref, velocity_ref,
     partner_ref, gap_ref, self_ref, pair_ref) = held
    (flow_ref, cols_ref, slip_ref, wide_ref, pick_ref, message_ref, got_ref, reply_ref, returned_ref,
     collided_ref, x_low_ref, x_high_ref, edge_out_ref, edge_in_ref, hot_ref, pairs_ref,
     load_sem, bulk_sem, own_sem, halo_send, halo_recv, row_sem) = rest
    slots, width = cell_ref.shape
    rows, depth = pops_ref.shape[1:]
    loads = [pltpu.make_async_copy(a, b, load_sem.at[n]) for n, (a, b) in enumerate(zip(given, held))]
    for load in loads:
        load.start()
    with scope("p0_greet"):
        greet()
    with scope("p0_load"):
        for load in loads:
            load.wait()
    with scope("p1_front"):
        send_slip((cell_ref, mcount_ref, pcount_ref, pid_ref, table_ref, velocity_ref, pops_ref,
                   flow_ref, cols_ref, slip_ref, wide_ref, pick_ref, message_ref, row_sem))
    with scope("p2_met"):
        met(row_sem)
    there = (message_ref, got_ref, bulk_sem.at[0], bulk_sem.at[1], own_sem.at[0], 8)
    with scope("p3_start"):
        exchange_start(*there)
    with scope("p3_mark"):
        pair_columns(partner_ref, gap_ref, pairs_ref)
        mark_depths(cell_ref, hot_ref, depth, 0)
    with scope("p4_wait"):
        exchange_wait(*there)
    with scope("p5_lub"):
        lubricate(got_ref, pairs_ref, self_ref, pair_ref, reply_ref, wide_ref)
    back = (reply_ref, returned_ref, bulk_sem.at[2], bulk_sem.at[3], own_sem.at[1], 6)
    with scope("p6_start"):
        exchange_start(*back)
    with scope("p7_mark"):
        mark_depths(cell_ref, hot_ref, depth, 1)
    with scope("p7_wait"):
        exchange_wait(*back)
    with scope("p8_unroute"):
        wide_ref[...] = returned_ref[...].astype(F32).reshape(wide_ref.shape)
        own = dot(pick_ref[...], take_rows(wide_ref), TN)
        live = iota((slots, width), 1).astype(F32) < cols_ref[:, 3:4]
        for c in range(3):
            value = jnp.where(live, own[:, c * width : (c + 1) * width], 0.0)
            slip_ref[c] = value
            marker_ref[c] = value.astype(BF16)
    with scope("p9_spread"):
        total = spread(cell_ref, slip_ref, hot_ref, rows, depth)
    with scope("pa_collide"):
        force = [total[c * rows : (c + 1) * rows] for c in range(3)]
        collide(pops_ref, force, collided_ref, ORDER)
        for n, i in enumerate(EDGES):
            at = rows - 1 if DIRS[i][1] == 1 else 0
            edge_out_ref[n] = collided_ref[PLACE[i], at : at + 1, :]
    copies = halo_copies(collided_ref, x_low_ref, x_high_ref, edge_out_ref, edge_in_ref, halo_send, halo_recv)
    for above, below in zip(copies[0:3], copies[3:6]):
        pl.when(neighbours()[0])(above.start)
        pl.when(neighbours()[1])(below.start)
    for copy in copies[6:]:
        copy.start()
    streams = (collided_ref, x_low_ref, x_high_ref, edge_in_ref, read_ref)
    inner = [0, 5, 6]
    with scope("pc_inner"):
        stream(inner, *streams)
    with scope("pd_hwait"):
        for above, below in zip(copies[0:3], copies[3:6]):

            @pl.when(neighbours()[0])
            def _():
                above.wait_send()
                below.wait_recv()

            @pl.when(neighbours()[1])
            def _():
                below.wait_send()
                above.wait_recv()

        for copy in copies[6:]:
            copy.wait()
    with scope("pe_stream"):
        stream([i for i in range(19) if i not in inner], *streams)


def per_device(
    populations, marker_cell, marker_count, particle_count, particle_id, owner_table,
    particle_velocity, pair_list, pair_gap, self_coupling, pair_coupling,
):
    rows, depth = populations.shape[2:]
    slots, width = marker_cell.shape[2:]
    slabs = lax.axis_size("slab")
    args = (
        populations[:, 0],
        marker_cell[0, 0],
        marker_count[0],
        particle_count,
        particle_id[0],
        owner_table,
        jnp.transpose(particle_velocity[0], (1, 0, 2)),
        jnp.transpose(pair_list[0, 0]),
        jnp.transpose(pair_gap[0, 0]),
        self_coupling,
        pair_coupling,
    )
    place = pl.BlockSpec(memory_space=pltpu.VMEM)
    post = ((slabs, 8, width), BF16)
    scratch = [
        ((2 * rows, depth), jnp.int32),
        ((slots, 8), F32),
        ((3, slots, width), F32),
        ((8 * slabs, width), F32),
        ((slots, slots), BF16),
        post,
        post,
        post,
        post,
        ((19, rows, depth), F32),
        ((5, rows, depth), F32),
        ((5, rows, depth), F32),
        ((10, 1, depth), F32),
        ((10, 1, depth), F32),
        ((slots // 8, 8 * width, depth), BF16),
        ((slots, 8), F32),
    ]
    held = [(arg.shape, arg.dtype) for arg in args]
    read, marker = pl.pallas_call(
        step_kernel,
        out_shape=[
            jax.ShapeDtypeStruct((19, rows, depth), F32),
            jax.ShapeDtypeStruct((3, slots, width), BF16),
        ],
        in_specs=[pl.BlockSpec(memory_space=pltpu.HBM)] * len(args),
        out_specs=[place] * 2,
        scratch_shapes=[pltpu.VMEM(shape, kind) for shape, kind in held + scratch]
        + [
            pltpu.SemaphoreType.DMA((len(args),)),
            pltpu.SemaphoreType.DMA((4,)),
            pltpu.SemaphoreType.DMA((2,)),
            pltpu.SemaphoreType.DMA((8,)),
            pltpu.SemaphoreType.DMA((8,)),
            pltpu.SemaphoreType.REGULAR,
        ],
        compiler_params=pltpu.CompilerParams(
            collective_id=0, has_side_effects=True, vmem_limit_bytes=VMEM_LIMIT
        ),
        name="step",
    )(*[pltpu.with_memory_space_constraint(arg, pltpu.HBM) if arg.size > 1 else arg for arg in args])
    return read[:, None], jnp.transpose(marker, (1, 0, 2))[None, None]


def solution(mesh):
    placed = (
        P(None, "slab", "sub", None),
        P("slab", "sub", None, None),
        P("slab", "sub", None),
        P("slab", "sub"),
        P("slab", "sub", None),
        P("sub", None),
        P("slab", "sub", None, None),
        P("slab", "sub", None, None),
        P("slab", "sub", None, None),
        P(),
        P(),
    )
    return jax.shard_map(
        per_device,
        mesh=mesh,
        in_specs=placed,
        out_specs=(P(None, "slab", "sub", None), P("slab", "sub", None, None, None)),
        check_vma=False,
    )
```

```python
import functools

import jax
import jax.numpy as jnp
from jax import lax
from jax.experimental import pallas as pl
from jax.experimental.pallas import tpu as pltpu
from jax.sharding import PartitionSpec as P

DIRS = [
    (0, 0, 0),
    (1, 0, 0),
    (-1, 0, 0),
    (0, 1, 0),
    (0, -1, 0),
    (0, 0, 1),
    (0, 0, -1),
    (1, 1, 0),
    (-1, -1, 0),
    (1, -1, 0),
    (-1, 1, 0),
    (1, 0, 1),
    (-1, 0, -1),
    (1, 0, -1),
    (-1, 0, 1),
    (0, 1, 1),
    (0, -1, -1),
    (0, 1, -1),
    (0, -1, 1),
]
WEIGHTS = [1.0 / 3.0] + [1.0 / 18.0] * 6 + [1.0 / 36.0] * 12
OPPOSITE = [0, 2, 1, 4, 3, 6, 5, 8, 7, 10, 9, 12, 11, 14, 13, 16, 15, 18, 17]
OMEGA = 1.25
SAMPLE_GROUP = 8
SPREAD_GROUP = 16
FIXED = float(1 << 21)
VMEM_LIMIT = 32 * 1024 * 1024
X_UP = [i for i in range(19) if DIRS[i][0] == 1]
X_DOWN = [i for i in range(19) if DIRS[i][0] == -1]
Y_UP = [i for i in range(19) if DIRS[i][1] == 1]
Y_DOWN = [i for i in range(19) if DIRS[i][1] == -1]

F32 = jnp.float32
BF16 = jnp.bfloat16
NN = (((1,), (0,)), ((), ()))
NT = (((1,), (1,)), ((), ()))
TN = (((0,), (0,)), ((), ()))


def dot(a, b, dims=NN):
    return lax.dot_general(a, b, dims, preferred_element_type=F32)


def iota(shape, axis):
    return lax.broadcasted_iota(jnp.int32, shape, axis)


def ones_at(mask):
    return jnp.where(mask, 1.0, 0.0).astype(BF16)


def split_cell(cell, depth):
    return cell & (depth - 1), lax.shift_right_logical(cell, depth.bit_length() - 1)


def split_two(value):
    high = value.astype(BF16)
    return high, (value - high.astype(F32)).astype(BF16)


def moments(pops_ref):
    pops = [pops_ref[i] for i in range(19)]
    density = functools.reduce(lambda a, b: a + b, pops)
    moment = []
    for c in range(3):
        up = functools.reduce(lambda a, b: a + b, [pops[i] for i in range(19) if DIRS[i][c] == 1])
        down = functools.reduce(lambda a, b: a + b, [pops[i] for i in range(19) if DIRS[i][c] == -1])
        moment.append(up - down)
    return density, moment


def flow_table(pops_ref, flow_ref):
    rows = pops_ref.shape[1]
    density, moment = moments(pops_ref)
    x, y, z = ((moment[c] / density * FIXED + 0.5 * FIXED + 0.5).astype(jnp.int32) for c in range(3))
    high = lax.shift_right_logical(z, 10)
    flow_ref[pl.ds(0, rows), :] = lax.shift_left(x, 11) + high
    flow_ref[pl.ds(rows, rows), :] = lax.shift_left(y, 11) + (z & 1023)


def unpack_flow(first, second):
    x = lax.shift_right_logical(first, 11)
    y = lax.shift_right_logical(second, 11)
    z = lax.shift_left(first & 2047, 10) + (second & 2047)
    return [value.astype(F32) * (1.0 / FIXED) - 0.5 for value in (x, y, z)]


def slot_columns(velocity_ref, mcount_ref, pcount_ref, cols_ref):
    slots = mcount_ref.shape[1]
    limit = jnp.where(iota((1, slots), 1) < pcount_ref[...], mcount_ref[...], 0).astype(F32)
    stack = [velocity_ref[...].reshape(3, slots), limit, jnp.zeros((4, slots), F32)]
    cols_ref[...] = jnp.concatenate(stack, axis=0).T


def routes(pid_ref, table_ref, pcount_ref, width):
    slots, slabs = pid_ref.shape[1], table_ref.shape[1]
    ids = pid_ref[...]
    alive = iota((1, slots), 1) < pcount_ref[...]
    in_range = ones_at(iota((slabs, slots), 0) == ids // slots)
    owner_of = ones_at(iota((slabs, slabs), 0) == table_ref[...])
    owner = jnp.where(alive, dot(owner_of, in_range), 0.0)
    before = ones_at(iota((slots, slots), 0) < iota((slots, slots), 1))
    earlier = dot(owner.astype(BF16), before)
    first = jnp.where(earlier < 0.5, owner, 0.0)
    pick = jnp.concatenate([first, owner - first], axis=0).astype(BF16)
    spot = (ids % slots + 1).astype(F32)
    spots = dot(pick, jnp.broadcast_to(spot, (width, slots)).astype(BF16), NT)
    return pick, spots


def sample(cell_ref, flow_ref, cols_ref, slip_ref, half):
    slots, width = cell_ref.shape
    rows = flow_ref.shape[0] // 2
    depth = flow_ref.shape[1]
    group = min(SAMPLE_GROUP, slots // 8)

    def block(g, carry):
        for n in range(group):
            at = pl.multiple_of(g * 8 * group + 8 * n, 8)
            z, y = split_cell(cell_ref[pl.ds(at, 8), :], depth)
            picked = [jnp.zeros((8, width), jnp.int32) for _ in range(2)]
            for row in range(rows):
                here = y == row
                for c in range(2):
                    line = jnp.broadcast_to(flow_ref[c * rows + row : c * rows + row + 1, :], (8, depth))
                    got = jnp.take_along_axis(line, z, axis=1, mode="promise_in_bounds")
                    picked[c] = jnp.where(here, got, picked[c])
            cols = cols_ref[pl.ds(at, 8), :]
            flow = unpack_flow(*picked)
            live = iota((8, width), 1).astype(F32) < cols[:, 3:4]
            for c in range(3):
                slip_ref[c, pl.ds(at, 8), :] = jnp.where(live, cols[:, c : c + 1] - flow[c], 0.0)
        return carry

    steps = slots // (8 * group)
    middle = steps // 2
    lax.fori_loop(middle if half else 0, steps if half else middle, block, 0)


def put_rows(wide_ref, rows, width):
    slabs = wide_ref.shape[0] // 8
    for p in range(2):
        for c in range(3):
            wide_ref[pl.ds(p * 3 + c, slabs, stride=8), :] = rows[
                p * slabs : (p + 1) * slabs, c * width : (c + 1) * width
            ]


def take_rows(wide_ref):
    slabs = wide_ref.shape[0] // 8
    sides = []
    for p in range(2):
        sides.append(
            jnp.concatenate(
                [wide_ref[pl.ds(p * 3 + c, slabs, stride=8), :] for c in range(3)], axis=1
            )
        )
    return jnp.concatenate(sides, axis=0).astype(BF16)


ORDER = X_UP + X_DOWN + [3, 4, 15, 16, 17, 18, 0, 5, 6]
PLACE = [ORDER.index(i) for i in range(19)]
EDGES = [3, 15, 17, 7, 10, 4, 16, 18, 9, 8]


def routed(mesh_ids):
    return dict(device_id=mesh_ids, device_id_type=pl.DeviceIdType.MESH)


def near_ids():
    slabs, subs = lax.axis_size("slab"), lax.axis_size("sub")
    me, side = lax.axis_index("slab"), lax.axis_index("sub")
    next_slab, last_slab = lax.rem(me + 1, slabs), lax.rem(me + slabs - 1, slabs)
    next_sub, last_sub = lax.rem(side + 1, subs), lax.rem(side + subs - 1, subs)
    return [
        {"slab": me, "sub": next_sub},
        {"slab": next_slab, "sub": next_sub},
        {"slab": last_slab, "sub": next_sub},
        {"slab": me, "sub": last_sub},
        {"slab": next_slab, "sub": last_sub},
        {"slab": last_slab, "sub": last_sub},
        {"slab": next_slab, "sub": side},
        {"slab": last_slab, "sub": side},
    ]


def inner_size():
    return 16 if lax.axis_size("slab") % 32 == 0 else 4


def neighbours():
    side = lax.axis_index("sub")
    return side < lax.axis_size("sub") - 1, side > 0


def greet():
    side = lax.axis_index("sub")
    barrier = pltpu.get_barrier_semaphore()
    for to in row_peers() + column_peers():
        pl.semaphore_signal(barrier, inc=1, **routed({"slab": to, "sub": side}))
    ids = near_ids()
    for beside, chosen in zip(neighbours(), (ids[0:3], ids[3:6])):

        @pl.when(beside)
        def _():
            for one in chosen:
                pl.semaphore_signal(barrier, inc=1, **routed(one))


def row_peers():
    inner, me = inner_size(), lax.axis_index("slab")
    base = me // inner * inner
    return [base + lax.rem(me + k, inner) for k in range(1, inner)]


def column_peers():
    slabs, inner, me = lax.axis_size("slab"), inner_size(), lax.axis_index("slab")
    return [lax.rem(me + k * inner, slabs) for k in range(1, slabs // inner)]


def relay(row_sem):
    side = lax.axis_index("sub")
    rows, columns = row_peers(), column_peers()
    last = lax.axis_size("sub") - 1
    beside = (side + last - 1) // last + (2 * last - 1 - side) // last
    pl.semaphore_wait(pltpu.get_barrier_semaphore(), len(rows) + len(columns) + 3 * beside)
    for to in columns:
        pl.semaphore_signal(row_sem, inc=1, **routed({"slab": to, "sub": side}))


def met(row_sem):
    pl.semaphore_wait(row_sem, len(column_peers()))


def far_first(size):
    return sorted(range(size), key=lambda step: -min(step, size - step))


def exchange_start(out_ref, in_ref, send_sem, recv_sem, own_sem, lines):
    slabs, inner = lax.axis_size("slab"), inner_size()
    outer, ring = slabs // inner, inner // 2
    me, side = lax.axis_index("slab"), lax.axis_index("sub")
    bases = [lax.rem(me // inner + step, outer) * inner for step in far_first(outer)]
    place = lax.rem(me, inner) // 2
    cores = [lax.rem(me + 1, 2), lax.rem(me, 2)]

    def send(to):
        pltpu.make_async_remote_copy(
            src_ref=out_ref.at[to, pl.ds(0, lines)],
            dst_ref=in_ref.at[me, pl.ds(0, lines)],
            send_sem=send_sem,
            recv_sem=recv_sem,
            **routed({"slab": to, "sub": side}),
        ).start()

    def one(j, carry):
        step = ring // 2 + (j + 1) // 2 * (1 - 2 * lax.rem(j + 1, 2))
        here = lax.rem(place + step, ring) * 2
        for base in bases:
            for core in cores:
                send(base + here + core)
        return carry

    lax.fori_loop(0, ring - 1, one, 0)
    for base in bases[:-1]:
        for core in cores:
            send(base + place * 2 + core)
    send(bases[-1] + place * 2 + cores[0])
    pltpu.make_async_copy(out_ref.at[me], in_ref.at[me], own_sem).start()


def exchange_wait(out_ref, in_ref, send_sem, recv_sem, own_sem, lines):
    slabs = lax.axis_size("slab")
    me = lax.axis_index("slab")
    others = pl.ds(0, slabs - 1)
    pltpu.make_async_copy(out_ref.at[me], in_ref.at[me], own_sem).wait()
    pltpu.make_async_copy(in_ref.at[others, pl.ds(0, lines)], in_ref.at[others, pl.ds(0, lines)], recv_sem).wait()
    pltpu.make_async_copy(out_ref.at[others, pl.ds(0, lines)], out_ref.at[others, pl.ds(0, lines)], send_sem).wait()


def halo_copies(collided_ref, x_low_ref, x_high_ref, edge_out_ref, edge_in_ref, send_sem, recv_sem):
    ids = near_ids()
    views = [(edge_out_ref.at[pl.ds(a, n)], edge_in_ref.at[pl.ds(a, n)]) for a, n in ((0, 3), (3, 1), (4, 1), (5, 3), (8, 1), (9, 1))]
    views.append((collided_ref.at[pl.ds(0, 5)], x_low_ref))
    views.append((collided_ref.at[pl.ds(5, 5)], x_high_ref))
    return [
        pltpu.make_async_remote_copy(
            src_ref=source,
            dst_ref=target,
            send_sem=send_sem.at[n],
            recv_sem=recv_sem.at[n],
            **routed(ids[n]),
        )
        for n, (source, target) in enumerate(views)
    ]


def scope(name):
    return jax.named_scope(name)


def send_slip(refs):
    (cell_ref, mcount_ref, pcount_ref, pid_ref, table_ref, velocity_ref, pops_ref,
     flow_ref, cols_ref, slip_ref, wide_ref, pick_ref, message_ref, row_sem, ready) = refs
    width = cell_ref.shape[1]
    slabs = message_ref.shape[0]
    with scope("q0_load"):
        ready(0, 5)
    with scope("q1_routes"):
        pick, spots = routes(pid_ref, table_ref, pcount_ref, width)
        pick_ref[...] = pick
        for p in range(2):
            wide_ref[pl.ds(6 + p, slabs, stride=8), :] = spots[p * slabs : (p + 1) * slabs]
    with scope("q3_cols"):
        slot_columns(velocity_ref, mcount_ref, pcount_ref, cols_ref)
    with scope("q3_load"):
        ready(5, 7)
    with scope("q2_flow"):
        flow_table(pops_ref, flow_ref)
    with scope("q4_sample"):
        sample(cell_ref, flow_ref, cols_ref, slip_ref, 0)
    with scope("q5_relay"):
        relay(row_sem)
    with scope("q6_sample"):
        sample(cell_ref, flow_ref, cols_ref, slip_ref, 1)
    slip = jnp.concatenate([slip_ref[c].astype(BF16) for c in range(3)], axis=1)
    put_rows(wide_ref, dot(pick_ref[...], slip), width)
    message_ref[...] = wide_ref[...].reshape(slabs, 8, width).astype(BF16)


def pair_columns(partner_ref, gap_ref, pairs_ref):
    pairs_ref[...] = jnp.concatenate([partner_ref[...].astype(F32) + 1.0, 1.0 / gap_ref[...]], axis=0).T


def lubricate(got_ref, pairs_ref, self_ref, pair_ref, reply_ref, wide_ref):
    slabs, _, width = got_ref.shape
    slots = 2 * slabs
    wide_ref[...] = got_ref[...].astype(F32).reshape(8 * slabs, width)
    owned = take_rows(wide_ref)
    spot_col = jnp.concatenate(
        [wide_ref[pl.ds(6 + p, slabs, stride=8), :] for p in range(2)], axis=0
    )
    head = ones_at(iota((slots, width), 1) == 0)
    spot_row = dot(head, spot_col.astype(BF16), NT)
    pairs = pairs_ref[...]
    weight = jnp.zeros((slots, slots), F32)
    for k in range(4):
        weight += jnp.where(pairs[:, k : k + 1] == spot_row, pairs[:, 4 + k : 5 + k], 0.0)
    high, low = split_two(weight)
    near = (dot(high, owned) + dot(low, owned)).astype(BF16)
    place = ones_at(spot_col[:, :1] - 1.0 == iota((slots, slots), 1).astype(F32))
    near = dot(place, near).astype(BF16)
    parts = []
    for c in range(3):
        side = slice(c * width, (c + 1) * width)
        parts.append(dot(owned[:, side], self_ref[...]) + dot(near[:, side], pair_ref[...]))
    put_rows(wide_ref, jnp.concatenate(parts, axis=1), width)
    reply_ref[...] = wide_ref[...].reshape(slabs, 8, width).astype(BF16)


def packed_row(value, j):
    return jnp.broadcast_to(value[j : j + 1, :], (16, value.shape[1])).astype(BF16)


def mark_depths(cell_ref, hot_ref, depth, half):
    slots, width = cell_ref.shape
    lanes = iota((width, depth), 1).astype(F32)

    def block(g, carry):
        z = split_cell(cell_ref[pl.ds(pl.multiple_of(g * 8, 8), 8), :], depth)[0].astype(F32).T
        for j in range(8):
            hot_ref[g, j * width : (j + 1) * width, :] = ones_at(z[:, j : j + 1] == lanes)
        return carry

    steps = slots // 8
    middle = steps // 2
    lax.fori_loop(middle if half else 0, steps if half else middle, block, 0)


def spread(cell_ref, force_ref, hot_ref, rows, depth):
    slots, width = cell_ref.shape
    lines = iota((16, width), 0).astype(F32).astype(BF16)
    zero = jnp.zeros((16, width), BF16)

    group = min(SPREAD_GROUP, slots // 8)

    def block(g, total):
        for n in range(group):
            at = pl.multiple_of(g * 8 * group + 8 * n, 8)
            y = split_cell(cell_ref[pl.ds(at, 8), :], depth)[1].astype(F32)
            vals = [force_ref[c, pl.ds(at, 8), :] for c in range(3)]
            sides = []
            for j in range(8):
                yb = packed_row(y, j)
                marks = [yb == lines + 16 * i for i in range(rows // 16)]
                stack = []
                for c in range(3):
                    vb = packed_row(vals[c], j)
                    stack += [jnp.where(mark, vb, zero) for mark in marks]
                sides.append(jnp.concatenate(stack, axis=0))
            total = total + dot(jnp.concatenate(sides, axis=1), hot_ref[g * group + n])
        return total

    return lax.fori_loop(0, slots // (8 * group), block, jnp.zeros((3 * rows, depth), F32))


def along(i, parts):
    terms = [parts[c] if DIRS[i][c] == 1 else -parts[c] for c in range(3) if DIRS[i][c] != 0]
    return functools.reduce(lambda a, b: a + b, terms) if terms else None


def collide(pops_ref, force, out_ref, chosen):
    density, moment = moments(pops_ref)
    inverse = 1.0 / density
    velocity = [(moment[c] + 0.5 * force[c]) * inverse for c in range(3)]
    speed_sq = velocity[0] * velocity[0] + velocity[1] * velocity[1] + velocity[2] * velocity[2]
    work = velocity[0] * force[0] + velocity[1] * force[1] + velocity[2] * force[2]
    base = 1.0 - 1.5 * speed_sq
    for i in chosen:
        w = WEIGHTS[i]
        cu, cf = along(i, velocity), along(i, force)
        if cu is None:
            equilibrium = w * density * base
            source = (1.0 - 0.5 * OMEGA) * w * (-3.0 * work)
        else:
            equilibrium = w * density * (base + 3.0 * cu + 4.5 * cu * cu)
            source = (1.0 - 0.5 * OMEGA) * w * (3.0 * (cf - work) + 9.0 * cu * cf)
        pops = pops_ref[i]
        out_ref[PLACE[i]] = pops - OMEGA * (pops - equilibrium) + source


def stream(chosen, collided_ref, x_low_ref, x_high_ref, edge_ref, read_ref):
    rows, depth = collided_ref.shape[1:]
    me = lax.axis_index("sub")
    last = lax.axis_size("sub") - 1
    row = iota((rows, depth), 0)
    for i in chosen:
        sx, sy, sz = DIRS[i]
        if sx == 0:
            value = collided_ref[PLACE[i]]
        elif sx == 1:
            value = x_low_ref[X_UP.index(i)]
        else:
            value = x_high_ref[X_DOWN.index(i)]
        if sy == 1:
            value = jnp.where(row == 0, edge_ref[EDGES.index(i)], pltpu.roll(value, 1, 0))
        elif sy == -1:
            value = jnp.where(row == rows - 1, edge_ref[EDGES.index(i)], pltpu.roll(value, rows - 1, 0))
        if sz != 0:
            value = pltpu.roll(value, sz % depth, 1)
        if sy != 0:
            wall_row, wall_device = (0, 0) if sy == 1 else (rows - 1, last)
            at_wall = (row == wall_row) & (me == wall_device)
            value = jnp.where(at_wall, collided_ref[PLACE[OPPOSITE[i]]], value)
        read_ref[i] = value


def step_kernel(*refs):
    given, (read_ref, marker_ref), rest = refs[:11], refs[11:13], refs[13:]
    held, rest = rest[:11], rest[11:]
    (mcount_ref, pcount_ref, pid_ref, table_ref, velocity_ref, pops_ref, cell_ref,
     partner_ref, gap_ref, self_ref, pair_ref) = held
    (flow_ref, cols_ref, slip_ref, wide_ref, pick_ref, message_ref, got_ref, reply_ref, returned_ref,
     collided_ref, x_low_ref, x_high_ref, edge_out_ref, edge_in_ref, hot_ref, pairs_ref,
     load_sem, bulk_sem, own_sem, halo_send, halo_recv, row_sem) = rest
    slots, width = cell_ref.shape
    rows, depth = pops_ref.shape[1:]
    loads = [pltpu.make_async_copy(a, b, load_sem.at[n]) for n, (a, b) in enumerate(zip(given, held))]
    for load in loads:
        load.start()
    with scope("p0_greet"):
        greet()

    def ready(first, last):
        for load in loads[first:last]:
            load.wait()

    with scope("p1_front"):
        send_slip((cell_ref, mcount_ref, pcount_ref, pid_ref, table_ref, velocity_ref, pops_ref,
                   flow_ref, cols_ref, slip_ref, wide_ref, pick_ref, message_ref, row_sem, ready))
    with scope("p2_met"):
        met(row_sem)
    there = (message_ref, got_ref, bulk_sem.at[0], bulk_sem.at[1], own_sem.at[0], 8)
    with scope("p3_start"):
        exchange_start(*there)
    with scope("p3_mark"):
        ready(7, 11)
        pair_columns(partner_ref, gap_ref, pairs_ref)
        mark_depths(cell_ref, hot_ref, depth, 0)
    with scope("p4_wait"):
        exchange_wait(*there)
    with scope("p5_lub"):
        lubricate(got_ref, pairs_ref, self_ref, pair_ref, reply_ref, wide_ref)
    back = (reply_ref, returned_ref, bulk_sem.at[2], bulk_sem.at[3], own_sem.at[1], 6)
    with scope("p6_start"):
        exchange_start(*back)
    with scope("p7_mark"):
        mark_depths(cell_ref, hot_ref, depth, 1)
    with scope("p7_wait"):
        exchange_wait(*back)
    with scope("p8_unroute"):
        wide_ref[...] = returned_ref[...].astype(F32).reshape(wide_ref.shape)
        own = dot(pick_ref[...], take_rows(wide_ref), TN)
        live = iota((slots, width), 1).astype(F32) < cols_ref[:, 3:4]
        for c in range(3):
            value = jnp.where(live, own[:, c * width : (c + 1) * width], 0.0)
            slip_ref[c] = value
            marker_ref[c] = value.astype(BF16)
    with scope("p9_spread"):
        total = spread(cell_ref, slip_ref, hot_ref, rows, depth)
    with scope("pa_collide"):
        force = [total[c * rows : (c + 1) * rows] for c in range(3)]
        collide(pops_ref, force, collided_ref, ORDER)
        for n, i in enumerate(EDGES):
            at = rows - 1 if DIRS[i][1] == 1 else 0
            edge_out_ref[n] = collided_ref[PLACE[i], at : at + 1, :]
    copies = halo_copies(collided_ref, x_low_ref, x_high_ref, edge_out_ref, edge_in_ref, halo_send, halo_recv)
    for above, below in zip(copies[0:3], copies[3:6]):
        pl.when(neighbours()[0])(above.start)
        pl.when(neighbours()[1])(below.start)
    for copy in copies[6:]:
        copy.start()
    streams = (collided_ref, x_low_ref, x_high_ref, edge_in_ref, read_ref)
    inner = [0, 5, 6]
    with scope("pc_inner"):
        stream(inner, *streams)
    with scope("pd_hwait"):
        for above, below in zip(copies[0:3], copies[3:6]):

            @pl.when(neighbours()[0])
            def _():
                above.wait_send()
                below.wait_recv()

            @pl.when(neighbours()[1])
            def _():
                below.wait_send()
                above.wait_recv()

        for copy in copies[6:]:
            copy.wait()
    with scope("pe_stream"):
        stream([i for i in range(19) if i not in inner], *streams)


def emit_kernel(read_ref, marker_ref, read_out, marker_out, sem):
    copies = [
        pltpu.make_async_copy(read_ref, read_out, sem.at[0]),
        pltpu.make_async_copy(marker_ref, marker_out, sem.at[1]),
    ]
    for copy in copies:
        copy.start()
    for copy in copies:
        copy.wait()


def per_device(
    populations, marker_cell, marker_count, particle_count, particle_id, owner_table,
    particle_velocity, pair_list, pair_gap, self_coupling, pair_coupling,
):
    rows, depth = populations.shape[2:]
    slots, width = marker_cell.shape[2:]
    slabs = lax.axis_size("slab")
    args = (
        marker_count[0],
        particle_count,
        particle_id[0],
        owner_table,
        jnp.transpose(particle_velocity[0], (1, 0, 2)),
        populations[:, 0],
        marker_cell[0, 0],
        jnp.transpose(pair_list[0, 0]),
        jnp.transpose(pair_gap[0, 0]),
        self_coupling,
        pair_coupling,
    )
    place = pl.BlockSpec(memory_space=pltpu.VMEM)
    post = ((slabs, 8, width), BF16)
    scratch = [
        ((2 * rows, depth), jnp.int32),
        ((slots, 8), F32),
        ((3, slots, width), F32),
        ((8 * slabs, width), F32),
        ((slots, slots), BF16),
        post,
        post,
        post,
        post,
        ((19, rows, depth), F32),
        ((5, rows, depth), F32),
        ((5, rows, depth), F32),
        ((10, 1, depth), F32),
        ((10, 1, depth), F32),
        ((slots // 8, 8 * width, depth), BF16),
        ((slots, 8), F32),
    ]
    held = [(arg.shape, arg.dtype) for arg in args]
    read, marker = pl.pallas_call(
        step_kernel,
        out_shape=[
            jax.ShapeDtypeStruct((19, rows, depth), F32),
            jax.ShapeDtypeStruct((3, slots, width), BF16),
        ],
        in_specs=[pl.BlockSpec(memory_space=pltpu.HBM)] * len(args),
        out_specs=[place] * 2,
        scratch_shapes=[pltpu.VMEM(shape, kind) for shape, kind in held + scratch]
        + [
            pltpu.SemaphoreType.DMA((len(args),)),
            pltpu.SemaphoreType.DMA((4,)),
            pltpu.SemaphoreType.DMA((2,)),
            pltpu.SemaphoreType.DMA((8,)),
            pltpu.SemaphoreType.DMA((8,)),
            pltpu.SemaphoreType.REGULAR,
        ],
        compiler_params=pltpu.CompilerParams(
            collective_id=0, has_side_effects=True, vmem_limit_bytes=VMEM_LIMIT
        ),
        name="step",
    )(*[pltpu.with_memory_space_constraint(arg, pltpu.HBM) if arg.size > 1 else arg for arg in args])
    read, marker = pl.pallas_call(
        emit_kernel,
        out_shape=[jax.ShapeDtypeStruct(part.shape, part.dtype) for part in (read, marker)],
        in_specs=[pl.BlockSpec(memory_space=pl.ANY)] * 2,
        out_specs=[pl.BlockSpec(memory_space=pl.ANY)] * 2,
        scratch_shapes=[pltpu.SemaphoreType.DMA((2,))],
        name="emit",
    )(*[pltpu.with_memory_space_constraint(part, pltpu.VMEM) for part in (read, marker)])
    return read[:, None], jnp.transpose(marker, (1, 0, 2))[None, None]


def solution(mesh):
    placed = (
        P(None, "slab", "sub", None),
        P("slab", "sub", None, None),
        P("slab", "sub", None),
        P("slab", "sub"),
        P("slab", "sub", None),
        P("sub", None),
        P("slab", "sub", None, None),
        P("slab", "sub", None, None),
        P("slab", "sub", None, None),
        P(),
        P(),
    )
    return jax.shard_map(
        per_device,
        mesh=mesh,
        in_specs=placed,
        out_specs=(P(None, "slab", "sub", None), P("slab", "sub", None, None, None)),
        check_vma=False,
    )
```

```python
import functools

import jax
import jax.numpy as jnp
from jax import lax
from jax.experimental import pallas as pl
from jax.experimental.pallas import tpu as pltpu
from jax.sharding import PartitionSpec as P

DIRS = [
    (0, 0, 0),
    (1, 0, 0),
    (-1, 0, 0),
    (0, 1, 0),
    (0, -1, 0),
    (0, 0, 1),
    (0, 0, -1),
    (1, 1, 0),
    (-1, -1, 0),
    (1, -1, 0),
    (-1, 1, 0),
    (1, 0, 1),
    (-1, 0, -1),
    (1, 0, -1),
    (-1, 0, 1),
    (0, 1, 1),
    (0, -1, -1),
    (0, 1, -1),
    (0, -1, 1),
]
WEIGHTS = [1.0 / 3.0] + [1.0 / 18.0] * 6 + [1.0 / 36.0] * 12
OPPOSITE = [0, 2, 1, 4, 3, 6, 5, 8, 7, 10, 9, 12, 11, 14, 13, 16, 15, 18, 17]
OMEGA = 1.25
SAMPLE_GROUP = 8
SPREAD_GROUP = 32
FIXED = float(1 << 21)
VMEM_LIMIT = 32 * 1024 * 1024
X_UP = [i for i in range(19) if DIRS[i][0] == 1]
X_DOWN = [i for i in range(19) if DIRS[i][0] == -1]
Y_UP = [i for i in range(19) if DIRS[i][1] == 1]
Y_DOWN = [i for i in range(19) if DIRS[i][1] == -1]

F32 = jnp.float32
BF16 = jnp.bfloat16
NN = (((1,), (0,)), ((), ()))
NT = (((1,), (1,)), ((), ()))
TN = (((0,), (0,)), ((), ()))


def dot(a, b, dims=NN):
    return lax.dot_general(a, b, dims, preferred_element_type=F32)


def iota(shape, axis):
    return lax.broadcasted_iota(jnp.int32, shape, axis)


def ones_at(mask):
    return jnp.where(mask, 1.0, 0.0).astype(BF16)


def split_cell(cell, depth):
    return cell & (depth - 1), lax.shift_right_logical(cell, depth.bit_length() - 1)


def split_two(value):
    high = value.astype(BF16)
    return high, (value - high.astype(F32)).astype(BF16)


def moments(pops_ref):
    pops = [pops_ref[i] for i in range(19)]
    density = functools.reduce(lambda a, b: a + b, pops)
    moment = []
    for c in range(3):
        up = functools.reduce(lambda a, b: a + b, [pops[i] for i in range(19) if DIRS[i][c] == 1])
        down = functools.reduce(lambda a, b: a + b, [pops[i] for i in range(19) if DIRS[i][c] == -1])
        moment.append(up - down)
    return density, moment


def flow_table(pops_ref, flow_ref):
    rows = pops_ref.shape[1]
    density, moment = moments(pops_ref)
    x, y, z = ((moment[c] / density * FIXED + 0.5 * FIXED + 0.5).astype(jnp.int32) for c in range(3))
    high = lax.shift_right_logical(z, 10)
    flow_ref[pl.ds(0, rows), :] = lax.shift_left(x, 11) + high
    flow_ref[pl.ds(rows, rows), :] = lax.shift_left(y, 11) + (z & 1023)


def unpack_flow(first, second):
    x = lax.shift_right_logical(first, 11)
    y = lax.shift_right_logical(second, 11)
    z = lax.shift_left(first & 2047, 10) + (second & 2047)
    return [value.astype(F32) * (1.0 / FIXED) - 0.5 for value in (x, y, z)]


def slot_columns(velocity_ref, mcount_ref, pcount_ref, cols_ref):
    slots = mcount_ref.shape[1]
    limit = jnp.where(iota((1, slots), 1) < pcount_ref[...], mcount_ref[...], 0).astype(F32)
    stack = [velocity_ref[...].reshape(3, slots), limit, jnp.zeros((4, slots), F32)]
    cols_ref[...] = jnp.concatenate(stack, axis=0).T


def routes(pid_ref, table_ref, pcount_ref, width):
    slots, slabs = pid_ref.shape[1], table_ref.shape[1]
    ids = pid_ref[...]
    alive = iota((1, slots), 1) < pcount_ref[...]
    in_range = ones_at(iota((slabs, slots), 0) == ids // slots)
    owner_of = ones_at(iota((slabs, slabs), 0) == table_ref[...])
    owner = jnp.where(alive, dot(owner_of, in_range), 0.0)
    before = ones_at(iota((slots, slots), 0) < iota((slots, slots), 1))
    earlier = dot(owner.astype(BF16), before)
    first = jnp.where(earlier < 0.5, owner, 0.0)
    pick = jnp.concatenate([first, owner - first], axis=0).astype(BF16)
    spot = (ids % slots + 1).astype(F32)
    spots = dot(pick, jnp.broadcast_to(spot, (width, slots)).astype(BF16), NT)
    return pick, spots


def sample(cell_ref, flow_ref, cols_ref, slip_ref, half):
    slots, width = cell_ref.shape
    rows = flow_ref.shape[0] // 2
    depth = flow_ref.shape[1]
    group = min(SAMPLE_GROUP, slots // 8)

    def block(g, carry):
        for n in range(group):
            at = pl.multiple_of(g * 8 * group + 8 * n, 8)
            z, y = split_cell(cell_ref[pl.ds(at, 8), :], depth)
            picked = [jnp.zeros((8, width), jnp.int32) for _ in range(2)]
            for row in range(rows):
                here = y == row
                for c in range(2):
                    line = jnp.broadcast_to(flow_ref[c * rows + row : c * rows + row + 1, :], (8, depth))
                    got = jnp.take_along_axis(line, z, axis=1, mode="promise_in_bounds")
                    picked[c] = jnp.where(here, got, picked[c])
            cols = cols_ref[pl.ds(at, 8), :]
            flow = unpack_flow(*picked)
            live = iota((8, width), 1).astype(F32) < cols[:, 3:4]
            for c in range(3):
                slip_ref[c, pl.ds(at, 8), :] = jnp.where(live, cols[:, c : c + 1] - flow[c], 0.0)
        return carry

    steps = slots // (8 * group)
    middle = steps // 2
    lax.fori_loop(middle if half else 0, steps if half else middle, block, 0)


def put_rows(wide_ref, rows, width):
    slabs = wide_ref.shape[0] // 8
    for p in range(2):
        for c in range(3):
            wide_ref[pl.ds(p * 3 + c, slabs, stride=8), :] = rows[
                p * slabs : (p + 1) * slabs, c * width : (c + 1) * width
            ]


def take_rows(wide_ref):
    slabs = wide_ref.shape[0] // 8
    sides = []
    for p in range(2):
        sides.append(
            jnp.concatenate(
                [wide_ref[pl.ds(p * 3 + c, slabs, stride=8), :] for c in range(3)], axis=1
            )
        )
    return jnp.concatenate(sides, axis=0).astype(BF16)


ORDER = X_UP + X_DOWN + [3, 4, 15, 16, 17, 18, 0, 5, 6]
PLACE = [ORDER.index(i) for i in range(19)]
EDGES = [3, 15, 17, 7, 10, 4, 16, 18, 9, 8]


def routed(mesh_ids):
    return dict(device_id=mesh_ids, device_id_type=pl.DeviceIdType.MESH)


def near_ids():
    slabs, subs = lax.axis_size("slab"), lax.axis_size("sub")
    me, side = lax.axis_index("slab"), lax.axis_index("sub")
    next_slab, last_slab = lax.rem(me + 1, slabs), lax.rem(me + slabs - 1, slabs)
    next_sub, last_sub = lax.rem(side + 1, subs), lax.rem(side + subs - 1, subs)
    return [
        {"slab": me, "sub": next_sub},
        {"slab": next_slab, "sub": next_sub},
        {"slab": last_slab, "sub": next_sub},
        {"slab": me, "sub": last_sub},
        {"slab": next_slab, "sub": last_sub},
        {"slab": last_slab, "sub": last_sub},
        {"slab": next_slab, "sub": side},
        {"slab": last_slab, "sub": side},
    ]


def inner_size():
    return 16 if lax.axis_size("slab") % 32 == 0 else 4


def neighbours():
    side = lax.axis_index("sub")
    return side < lax.axis_size("sub") - 1, side > 0


def greet():
    side = lax.axis_index("sub")
    barrier = pltpu.get_barrier_semaphore()
    for to in row_peers() + column_peers():
        pl.semaphore_signal(barrier, inc=1, **routed({"slab": to, "sub": side}))
    ids = near_ids()
    for beside, chosen in zip(neighbours(), (ids[0:3], ids[3:6])):

        @pl.when(beside)
        def _():
            for one in chosen:
                pl.semaphore_signal(barrier, inc=1, **routed(one))


def row_peers():
    inner, me = inner_size(), lax.axis_index("slab")
    base = me // inner * inner
    return [base + lax.rem(me + k, inner) for k in range(1, inner)]


def column_peers():
    slabs, inner, me = lax.axis_size("slab"), inner_size(), lax.axis_index("slab")
    return [lax.rem(me + k * inner, slabs) for k in range(1, slabs // inner)]


def relay(row_sem):
    side = lax.axis_index("sub")
    rows, columns = row_peers(), column_peers()
    last = lax.axis_size("sub") - 1
    beside = (side + last - 1) // last + (2 * last - 1 - side) // last
    pl.semaphore_wait(pltpu.get_barrier_semaphore(), len(rows) + len(columns) + 3 * beside)
    for to in columns:
        pl.semaphore_signal(row_sem, inc=1, **routed({"slab": to, "sub": side}))


def met(row_sem):
    pl.semaphore_wait(row_sem, len(column_peers()))


def far_first(size):
    return sorted(range(size), key=lambda step: -min(step, size - step))


def exchange_start(out_ref, in_ref, send_sem, recv_sem, own_sem, lines):
    slabs, inner = lax.axis_size("slab"), inner_size()
    outer, ring = slabs // inner, inner // 2
    me, side = lax.axis_index("slab"), lax.axis_index("sub")
    bases = [lax.rem(me // inner + step, outer) * inner for step in far_first(outer)]
    place = lax.rem(me, inner) // 2
    cores = [lax.rem(me + 1, 2), lax.rem(me, 2)]

    def send(to):
        pltpu.make_async_remote_copy(
            src_ref=out_ref.at[to, pl.ds(0, lines)],
            dst_ref=in_ref.at[me, pl.ds(0, lines)],
            send_sem=send_sem,
            recv_sem=recv_sem,
            **routed({"slab": to, "sub": side}),
        ).start()

    def one(j, carry):
        step = ring // 2 + (j + 1) // 2 * (1 - 2 * lax.rem(j + 1, 2))
        here = lax.rem(place + step, ring) * 2
        for base in bases:
            for core in cores:
                send(base + here + core)
        return carry

    lax.fori_loop(0, ring - 1, one, 0)
    for base in bases[:-1]:
        for core in cores:
            send(base + place * 2 + core)
    send(bases[-1] + place * 2 + cores[0])
    pltpu.make_async_copy(out_ref.at[me], in_ref.at[me], own_sem).start()


def exchange_wait(out_ref, in_ref, send_sem, recv_sem, own_sem, lines):
    slabs = lax.axis_size("slab")
    me = lax.axis_index("slab")
    others = pl.ds(0, slabs - 1)
    pltpu.make_async_copy(out_ref.at[me], in_ref.at[me], own_sem).wait()
    pltpu.make_async_copy(in_ref.at[others, pl.ds(0, lines)], in_ref.at[others, pl.ds(0, lines)], recv_sem).wait()
    pltpu.make_async_copy(out_ref.at[others, pl.ds(0, lines)], out_ref.at[others, pl.ds(0, lines)], send_sem).wait()


def halo_copies(collided_ref, x_low_ref, x_high_ref, edge_out_ref, edge_in_ref, send_sem, recv_sem):
    ids = near_ids()
    views = [(edge_out_ref.at[pl.ds(a, n)], edge_in_ref.at[pl.ds(a, n)]) for a, n in ((0, 3), (3, 1), (4, 1), (5, 3), (8, 1), (9, 1))]
    views.append((collided_ref.at[pl.ds(0, 5)], x_low_ref))
    views.append((collided_ref.at[pl.ds(5, 5)], x_high_ref))
    return [
        pltpu.make_async_remote_copy(
            src_ref=source,
            dst_ref=target,
            send_sem=send_sem.at[n],
            recv_sem=recv_sem.at[n],
            **routed(ids[n]),
        )
        for n, (source, target) in enumerate(views)
    ]


def scope(name):
    return jax.named_scope(name)


def send_slip(refs):
    (cell_ref, mcount_ref, pcount_ref, pid_ref, table_ref, velocity_ref, pops_ref,
     flow_ref, cols_ref, slip_ref, wide_ref, pick_ref, message_ref, row_sem, ready) = refs
    width = cell_ref.shape[1]
    slabs = message_ref.shape[0]
    with scope("q0_load"):
        ready(0, 5)
    with scope("q1_routes"):
        pick, spots = routes(pid_ref, table_ref, pcount_ref, width)
        pick_ref[...] = pick
        for p in range(2):
            wide_ref[pl.ds(6 + p, slabs, stride=8), :] = spots[p * slabs : (p + 1) * slabs]
    with scope("q3_cols"):
        slot_columns(velocity_ref, mcount_ref, pcount_ref, cols_ref)
    with scope("q3_load"):
        ready(5, 7)
    with scope("q2_flow"):
        flow_table(pops_ref, flow_ref)
    with scope("q4_sample"):
        sample(cell_ref, flow_ref, cols_ref, slip_ref, 0)
    with scope("q5_relay"):
        relay(row_sem)
    with scope("q6_sample"):
        sample(cell_ref, flow_ref, cols_ref, slip_ref, 1)
    slip = jnp.concatenate([slip_ref[c].astype(BF16) for c in range(3)], axis=1)
    put_rows(wide_ref, dot(pick_ref[...], slip), width)
    message_ref[...] = wide_ref[...].reshape(slabs, 8, width).astype(BF16)


def pair_columns(partner_ref, gap_ref, pairs_ref):
    pairs_ref[...] = jnp.concatenate([partner_ref[...].astype(F32) + 1.0, 1.0 / gap_ref[...]], axis=0).T


def lubricate(got_ref, pairs_ref, self_ref, pair_ref, reply_ref, wide_ref):
    slabs, _, width = got_ref.shape
    slots = 2 * slabs
    wide_ref[...] = got_ref[...].astype(F32).reshape(8 * slabs, width)
    owned = take_rows(wide_ref)
    spot_col = jnp.concatenate(
        [wide_ref[pl.ds(6 + p, slabs, stride=8), :] for p in range(2)], axis=0
    )
    head = ones_at(iota((slots, width), 1) == 0)
    spot_row = dot(head, spot_col.astype(BF16), NT)
    pairs = pairs_ref[...]
    weight = jnp.zeros((slots, slots), F32)
    for k in range(4):
        weight += jnp.where(pairs[:, k : k + 1] == spot_row, pairs[:, 4 + k : 5 + k], 0.0)
    high, low = split_two(weight)
    near = (dot(high, owned) + dot(low, owned)).astype(BF16)
    place = ones_at(spot_col[:, :1] - 1.0 == iota((slots, slots), 1).astype(F32))
    near = dot(place, near).astype(BF16)
    parts = []
    for c in range(3):
        side = slice(c * width, (c + 1) * width)
        parts.append(dot(owned[:, side], self_ref[...]) + dot(near[:, side], pair_ref[...]))
    put_rows(wide_ref, jnp.concatenate(parts, axis=1), width)
    reply_ref[...] = wide_ref[...].reshape(slabs, 8, width).astype(BF16)


def packed_row(value, j):
    return jnp.broadcast_to(value[j : j + 1, :], (16, value.shape[1])).astype(BF16)


def mark_depths(cell_ref, hot_ref, depth, half):
    slots, width = cell_ref.shape
    lanes = iota((width, depth), 1).astype(F32)

    def block(g, carry):
        z = split_cell(cell_ref[pl.ds(pl.multiple_of(g * 8, 8), 8), :], depth)[0].astype(F32).T
        for j in range(8):
            hot_ref[g, j * width : (j + 1) * width, :] = ones_at(z[:, j : j + 1] == lanes)
        return carry

    steps = slots // 8
    middle = steps // 2
    lax.fori_loop(middle if half else 0, steps if half else middle, block, 0)


def spread(cell_ref, force_ref, hot_ref, rows, depth):
    slots, width = cell_ref.shape
    lines = iota((16, width), 0).astype(F32).astype(BF16)
    zero = jnp.zeros((16, width), BF16)

    group = min(SPREAD_GROUP, slots // 8)

    def block(g, total):
        for n in range(group):
            at = pl.multiple_of(g * 8 * group + 8 * n, 8)
            y = split_cell(cell_ref[pl.ds(at, 8), :], depth)[1].astype(F32)
            vals = [force_ref[c, pl.ds(at, 8), :] for c in range(3)]
            sides = []
            for j in range(8):
                yb = packed_row(y, j)
                marks = [yb == lines + 16 * i for i in range(rows // 16)]
                stack = []
                for c in range(3):
                    vb = packed_row(vals[c], j)
                    stack += [jnp.where(mark, vb, zero) for mark in marks]
                sides.append(jnp.concatenate(stack, axis=0))
            total = total + dot(jnp.concatenate(sides, axis=1), hot_ref[g * group + n])
        return total

    return lax.fori_loop(0, slots // (8 * group), block, jnp.zeros((3 * rows, depth), F32))


def along(i, parts):
    terms = [parts[c] if DIRS[i][c] == 1 else -parts[c] for c in range(3) if DIRS[i][c] != 0]
    return functools.reduce(lambda a, b: a + b, terms) if terms else None


def collide(pops_ref, force, out_ref, chosen):
    density, moment = moments(pops_ref)
    inverse = 1.0 / density
    velocity = [(moment[c] + 0.5 * force[c]) * inverse for c in range(3)]
    speed_sq = velocity[0] * velocity[0] + velocity[1] * velocity[1] + velocity[2] * velocity[2]
    work = velocity[0] * force[0] + velocity[1] * force[1] + velocity[2] * force[2]
    base = 1.0 - 1.5 * speed_sq
    for i in chosen:
        w = WEIGHTS[i]
        cu, cf = along(i, velocity), along(i, force)
        if cu is None:
            equilibrium = w * density * base
            source = (1.0 - 0.5 * OMEGA) * w * (-3.0 * work)
        else:
            equilibrium = w * density * (base + 3.0 * cu + 4.5 * cu * cu)
            source = (1.0 - 0.5 * OMEGA) * w * (3.0 * (cf - work) + 9.0 * cu * cf)
        pops = pops_ref[i]
        out_ref[PLACE[i]] = pops - OMEGA * (pops - equilibrium) + source


def stream(chosen, collided_ref, x_low_ref, x_high_ref, edge_ref, read_ref):
    rows, depth = collided_ref.shape[1:]
    me = lax.axis_index("sub")
    last = lax.axis_size("sub") - 1
    row = iota((rows, depth), 0)
    for i in chosen:
        sx, sy, sz = DIRS[i]
        if sx == 0:
            value = collided_ref[PLACE[i]]
        elif sx == 1:
            value = x_low_ref[X_UP.index(i)]
        else:
            value = x_high_ref[X_DOWN.index(i)]
        if sy == 1:
            value = jnp.where(row == 0, edge_ref[EDGES.index(i)], pltpu.roll(value, 1, 0))
        elif sy == -1:
            value = jnp.where(row == rows - 1, edge_ref[EDGES.index(i)], pltpu.roll(value, rows - 1, 0))
        if sz != 0:
            value = pltpu.roll(value, sz % depth, 1)
        if sy != 0:
            wall_row, wall_device = (0, 0) if sy == 1 else (rows - 1, last)
            at_wall = (row == wall_row) & (me == wall_device)
            value = jnp.where(at_wall, collided_ref[PLACE[OPPOSITE[i]]], value)
        read_ref[i] = value


def step_kernel(*refs):
    given, (read_ref, marker_ref), rest = refs[:11], refs[11:13], refs[13:]
    held, rest = rest[:11], rest[11:]
    (mcount_ref, pcount_ref, pid_ref, table_ref, velocity_ref, pops_ref, cell_ref,
     partner_ref, gap_ref, self_ref, pair_ref) = held
    (flow_ref, cols_ref, slip_ref, wide_ref, pick_ref, message_ref, got_ref, reply_ref, returned_ref,
     collided_ref, x_low_ref, x_high_ref, edge_out_ref, edge_in_ref, hot_ref, pairs_ref,
     load_sem, bulk_sem, own_sem, halo_send, halo_recv, row_sem) = rest
    slots, width = cell_ref.shape
    rows, depth = pops_ref.shape[1:]
    loads = [pltpu.make_async_copy(a, b, load_sem.at[n]) for n, (a, b) in enumerate(zip(given, held))]
    for load in loads:
        load.start()
    with scope("p0_greet"):
        greet()

    def ready(first, last):
        for load in loads[first:last]:
            load.wait()

    with scope("p1_front"):
        send_slip((cell_ref, mcount_ref, pcount_ref, pid_ref, table_ref, velocity_ref, pops_ref,
                   flow_ref, cols_ref, slip_ref, wide_ref, pick_ref, message_ref, row_sem, ready))
    with scope("p2_met"):
        met(row_sem)
    there = (message_ref, got_ref, bulk_sem.at[0], bulk_sem.at[1], own_sem.at[0], 8)
    with scope("p3_start"):
        exchange_start(*there)
    with scope("p3_mark"):
        ready(7, 11)
        pair_columns(partner_ref, gap_ref, pairs_ref)
        mark_depths(cell_ref, hot_ref, depth, 0)
    with scope("p4_wait"):
        exchange_wait(*there)
    with scope("p5_lub"):
        lubricate(got_ref, pairs_ref, self_ref, pair_ref, reply_ref, wide_ref)
    back = (reply_ref, returned_ref, bulk_sem.at[2], bulk_sem.at[3], own_sem.at[1], 6)
    with scope("p6_start"):
        exchange_start(*back)
    with scope("p7_mark"):
        mark_depths(cell_ref, hot_ref, depth, 1)
    with scope("p7_wait"):
        exchange_wait(*back)
    with scope("p8_unroute"):
        wide_ref[...] = returned_ref[...].astype(F32).reshape(wide_ref.shape)
        own = dot(pick_ref[...], take_rows(wide_ref), TN)
        live = iota((slots, width), 1).astype(F32) < cols_ref[:, 3:4]
        for c in range(3):
            value = jnp.where(live, own[:, c * width : (c + 1) * width], 0.0)
            slip_ref[c] = value
            marker_ref[c] = value.astype(BF16)
    with scope("p9_spread"):
        total = spread(cell_ref, slip_ref, hot_ref, rows, depth)
    with scope("pa_collide"):
        force = [total[c * rows : (c + 1) * rows] for c in range(3)]
        collide(pops_ref, force, collided_ref, ORDER)
        for n, i in enumerate(EDGES):
            at = rows - 1 if DIRS[i][1] == 1 else 0
            edge_out_ref[n] = collided_ref[PLACE[i], at : at + 1, :]
    copies = halo_copies(collided_ref, x_low_ref, x_high_ref, edge_out_ref, edge_in_ref, halo_send, halo_recv)
    for above, below in zip(copies[0:3], copies[3:6]):
        pl.when(neighbours()[0])(above.start)
        pl.when(neighbours()[1])(below.start)
    for copy in copies[6:]:
        copy.start()
    streams = (collided_ref, x_low_ref, x_high_ref, edge_in_ref, read_ref)
    inner = [0, 5, 6]
    with scope("pc_inner"):
        stream(inner, *streams)
    with scope("pd_hwait"):
        for above, below in zip(copies[0:3], copies[3:6]):

            @pl.when(neighbours()[0])
            def _():
                above.wait_send()
                below.wait_recv()

            @pl.when(neighbours()[1])
            def _():
                below.wait_send()
                above.wait_recv()

        for copy in copies[6:]:
            copy.wait()
    with scope("pe_stream"):
        stream([i for i in range(19) if i not in inner], *streams)


def emit_kernel(read_ref, marker_ref, read_out, marker_out, sem):
    copies = [
        pltpu.make_async_copy(read_ref, read_out, sem.at[0]),
        pltpu.make_async_copy(marker_ref, marker_out, sem.at[1]),
    ]
    for copy in copies:
        copy.start()
    for copy in copies:
        copy.wait()


def per_device(
    populations, marker_cell, marker_count, particle_count, particle_id, owner_table,
    particle_velocity, pair_list, pair_gap, self_coupling, pair_coupling,
):
    rows, depth = populations.shape[2:]
    slots, width = marker_cell.shape[2:]
    slabs = lax.axis_size("slab")
    args = (
        marker_count[0],
        particle_count,
        particle_id[0],
        owner_table,
        jnp.transpose(particle_velocity[0], (1, 0, 2)),
        populations[:, 0],
        marker_cell[0, 0],
        jnp.transpose(pair_list[0, 0]),
        jnp.transpose(pair_gap[0, 0]),
        self_coupling,
        pair_coupling,
    )
    place = pl.BlockSpec(memory_space=pltpu.VMEM)
    post = ((slabs, 8, width), BF16)
    scratch = [
        ((2 * rows, depth), jnp.int32),
        ((slots, 8), F32),
        ((3, slots, width), F32),
        ((8 * slabs, width), F32),
        ((slots, slots), BF16),
        post,
        post,
        post,
        post,
        ((19, rows, depth), F32),
        ((5, rows, depth), F32),
        ((5, rows, depth), F32),
        ((10, 1, depth), F32),
        ((10, 1, depth), F32),
        ((slots // 8, 8 * width, depth), BF16),
        ((slots, 8), F32),
    ]
    held = [(arg.shape, arg.dtype) for arg in args]
    read, marker = pl.pallas_call(
        step_kernel,
        out_shape=[
            jax.ShapeDtypeStruct((19, rows, depth), F32),
            jax.ShapeDtypeStruct((3, slots, width), BF16),
        ],
        in_specs=[pl.BlockSpec(memory_space=pltpu.HBM)] * len(args),
        out_specs=[place] * 2,
        scratch_shapes=[pltpu.VMEM(shape, kind) for shape, kind in held + scratch]
        + [
            pltpu.SemaphoreType.DMA((len(args),)),
            pltpu.SemaphoreType.DMA((4,)),
            pltpu.SemaphoreType.DMA((2,)),
            pltpu.SemaphoreType.DMA((8,)),
            pltpu.SemaphoreType.DMA((8,)),
            pltpu.SemaphoreType.REGULAR,
        ],
        compiler_params=pltpu.CompilerParams(
            collective_id=0, has_side_effects=True, vmem_limit_bytes=VMEM_LIMIT
        ),
        name="step",
    )(*[pltpu.with_memory_space_constraint(arg, pltpu.HBM) if arg.size > 1 else arg for arg in args])
    read, marker = pl.pallas_call(
        emit_kernel,
        out_shape=[jax.ShapeDtypeStruct(part.shape, part.dtype) for part in (read, marker)],
        in_specs=[pl.BlockSpec(memory_space=pl.ANY)] * 2,
        out_specs=[pl.BlockSpec(memory_space=pl.ANY)] * 2,
        scratch_shapes=[pltpu.SemaphoreType.DMA((2,))],
        name="emit",
    )(*[pltpu.with_memory_space_constraint(part, pltpu.VMEM) for part in (read, marker)])
    return read[:, None], jnp.transpose(marker, (1, 0, 2))[None, None]


def solution(mesh):
    placed = (
        P(None, "slab", "sub", None),
        P("slab", "sub", None, None),
        P("slab", "sub", None),
        P("slab", "sub"),
        P("slab", "sub", None),
        P("sub", None),
        P("slab", "sub", None, None),
        P("slab", "sub", None, None),
        P("slab", "sub", None, None),
        P(),
        P(),
    )
    return jax.shard_map(
        per_device,
        mesh=mesh,
        in_specs=placed,
        out_specs=(P(None, "slab", "sub", None), P("slab", "sub", None, None, None)),
        check_vma=False,
    )
```
